32 devices in a mesh: row: 4 (over x, core), col: 4 (over z), inner: 2 (over y).
Axes of the slice: x: 2, y: 2, z: 4, core: 2. Of those that a mesh axis runs over, the one named last changes fastest.
Arguments:
- near_flags: int32 [4, 6], P('row', 'inner'), may hold values 0 or 1
- row_factor: bfloat16 [4, 6, 64, 2048], P('row', 'inner', None, 'col'), may hold values from -6 to 6
- col_factor: bfloat16 [4, 6, 64, 2048], P('row', 'inner', None, 'col'), may hold values from -0.0068359375 to 0.0068359375
- near_block: bfloat16 [4, 6, 2048, 2048], P('row', 'inner', None, 'col'), may hold values from -0.0546875 to 0.0546875
- inner_left: bfloat16 [6, 16, 64, 2048], P('inner', 'col', None, 'row'), may hold values from -6 to 6
- inner_right: bfloat16 [6, 16, 64, 2048], P('inner', 'col', None, 'row'), may hold values from -0.75 to 0.75
- sketch_matrix: bfloat16 [16, 64, 2048], P('col'), may hold values from -0.125 to 0.125
Outputs:
- basis: float32 [4, 16, 64, 2048], P('row', 'col', None, 'inner')
- coupling: float32 [4, 16, 64, 2048], P('row', 'col', None, 'inner')
The draws below stay inside these ranges and needn't reach their ends.
Inputs may be any that keep to these rules, and one draw needn't show every extreme that they name: `near_flags`: 1 marks a near-field block.
All inputs are finite; a program needn't handle non-finite values.
Results may differ from the reference program's by a relative error of at most 0.0055.
Values may be sent and summed in bfloat16 or wider, within the bound.
A program may use at most 128 MiB of HBM per device.

```python
import math
import jax
import jax.numpy as jnp
from jax import lax

L = 2048
R = 64
K_I = 4
K_J = 16
K_K = 6


def set_ends(values, rng, least, top_value):
    place = [jax.random.randint(jax.random.fold_in(rng, axis), (), 0, length) for axis, length in enumerate(values.shape)]
    main_axis = values.shape.index(max(values.shape))
    next_to = place[:main_axis] + [(place[main_axis] + 1) % values.shape[main_axis]] + place[main_axis + 1:]
    return values.at[tuple(place)].set(least).at[tuple(next_to)].set(top_value)


def level_of(key, dims, split, smallest, high):
    def one(axis_at, parts):
        steps = jax.random.uniform(jax.random.fold_in(jax.random.fold_in(key, 6), axis_at), (parts,), jnp.float32, smallest / len(split), high / len(split))
        return jnp.repeat(jnp.exp(steps), dims[axis_at] // parts).reshape((-1,) + (1,) * (len(dims) - axis_at - 1))

    factor_of = one(*split[0])
    for cut in split[1:]:
        factor_of = factor_of * one(*cut)
    return factor_of


def scatter_about(rng, dims, scale, bound, cuts=(), dtype=jnp.bfloat16):
    drawn = jax.random.normal(rng, dims, jnp.float32) * scale
    if len(cuts) > 0:
        drawn = level_of(rng, dims, cuts, -0.22, 0.18) * drawn
    return jnp.clip(drawn, min=-bound, max=bound).astype(dtype)


def setup_inputs(seed: int = 0) -> dict:
    splits = jax.random.split(jax.random.key(seed), 8)
    near_flags = set_ends((jax.random.randint(splits[0], (K_I, K_K), 0, 2) < 1).astype(jnp.int32), jax.random.fold_in(splits[0], 1), 0, 1)
    row_factor = scatter_about(splits[1], (K_I, K_K, R, L), 1.0, 6.0, ((0, 4), (1, 2), (3, 4)))
    col_factor = scatter_about(splits[2], (K_I, K_K, R, L), (R * L * K_K) ** -0.5, 0.0068359375, ((0, 4), (1, 2), (3, 4)))
    near_block = scatter_about(splits[3], (K_I, K_K, L, L), (L * K_K) ** -0.5, 0.0546875, ((0, 4), (1, 2), (3, 4)))
    inner_left = scatter_about(splits[4], (K_K, K_J, R, L), 1.0, 6.0, ((0, 2), (1, 4), (3, 4)))
    inner_right = scatter_about(splits[5], (K_K, K_J, R, L), R ** -0.5, 0.75, ((0, 2), (1, 4), (3, 4)))
    sketch_matrix = scatter_about(splits[6], (K_J, R, L), L ** -0.5, 0.125, ((0, 4),))
    return dict(near_flags=near_flags, row_factor=row_factor, col_factor=col_factor, near_block=near_block, inner_left=inner_left, inner_right=inner_right, sketch_matrix=sketch_matrix)


def solve_lower(lower, sampled):
    return jax.scipy.linalg.solve_triangular(lower, sampled, lower=True)

def reference(near_flags, row_factor, col_factor, near_block, inner_left, inner_right, sketch_matrix):
    wide = jnp.float32
    narrow = jnp.bfloat16
    highest = lax.Precision.HIGHEST
    reduced = jnp.einsum('kjrl,jsl->kjrs', inner_right.astype(wide), sketch_matrix.astype(wide)).astype(narrow)
    right_wide = inner_right.astype(wide)

    def block_row(operands):
        rows_i, cols_i, dense_i, flags_i = operands

        def one_block(inner_ops):
            rows_k, cols_k, dense_k, flag_k, left_k = inner_ops

            def lowrank(unused):
                coupled = jnp.einsum('rl,jsl->jrs', cols_k.astype(wide), left_k.astype(wide)).astype(narrow)
                return jnp.einsum('jrs,rl->jsl', coupled.astype(wide), rows_k.astype(wide))

            def neardense(unused):
                flat = left_k.reshape(K_J * R, L)
                return jnp.dot(flat, dense_k, preferred_element_type=wide).reshape(K_J, R, L)
            return lax.cond(flag_k > 0, neardense, lowrank, 0).astype(narrow)
        pieces = lax.map(one_block, (rows_i, cols_i, dense_i, flags_i, inner_left))
        pieces_wide = pieces.astype(wide)
        sampled = jnp.einsum('kjrs,kjrl->jsl', reduced.astype(wide), pieces_wide)
        gram_matrix = jnp.einsum('jsl,jtl->jst', sampled, sampled, precision=highest) / L
        lower = jnp.linalg.cholesky(gram_matrix)
        basis = jax.vmap(solve_lower)(lower, sampled)
        projected = jnp.einsum('kjrl,jsl->kjrs', pieces_wide, basis, precision=highest) / math.sqrt(L)
        coupling = jnp.einsum('kjrs,kjrl->jsl', projected, right_wide, precision=highest)
        return (basis, coupling)
    basis, coupling = lax.map(block_row, (row_factor, col_factor, near_block, near_flags))
    return (basis, coupling)
```

```python
import functools
import math

import jax
import jax.numpy as jnp
from jax import lax
from jax.experimental import pallas as pl
from jax.experimental.pallas import tpu as pltpu
from jax.sharding import PartitionSpec as P

MESH = pl.DeviceIdType.MESH
HIGHEST = lax.Precision.HIGHEST
WIDE = jnp.float32
NARROW = jnp.bfloat16
NT = (((1,), (1,)), ((), ()))
TN = (((0,), (0,)), ((), ()))


def remote(src, dst, send, recv, device):
    return pltpu.make_async_remote_copy(
        src_ref=src, dst_ref=dst, send_sem=send, recv_sem=recv, device_id=device, device_id_type=MESH
    )


def meet(devices):
    barrier = pltpu.get_barrier_semaphore()
    for device in devices:
        pl.semaphore_signal(barrier, inc=1, device_id=device, device_id_type=MESH)
    pl.semaphore_wait(barrier, len(devices))


def split(value):
    high = value.astype(NARROW)
    return high, (value - high.astype(WIDE)).astype(NARROW)


def lanes(length):
    return -(-length // 128) * 128


def product_kernel(
    dims, mask_ref, u_ref, v_ref, d_ref, x_ref, y_ref, o_ref,
    s_home, cross_out, gram_out, yg,
    xg, vg, deff, pbuf, zt, zpart, zgot, zown, spart, ssend, sgot, msend, mgot, hsend,
    x_z_send, x_z_recv, x_f_send, x_f_recv, x_t_send, x_t_recv,
    v_send, v_recv, z_z_send, z_z_recv, z_f_send, z_f_recv, z_t_send, z_t_recv, zp_send, zp_recv,
    s_send, s_recv, m_send, m_recv, h_send, h_recv, y_f_send, y_f_recv, y_t_send, y_t_recv, own,
):
    n_row, n_col, n_in, slots, own_j, rank, width, cols = dims
    js = own_j * rank
    kr = slots * rank
    group = n_col // n_in
    planes = n_row // 2
    zrows = js // n_row
    row, col, inner = lax.axis_index("row"), lax.axis_index("col"), lax.axis_index("inner")
    plane = lax.div(row, 2)
    parity = lax.rem(row, 2)
    twin = {"row": row + 1 - 2 * parity}
    far_planes = [lax.rem(plane + f, planes) for f in range(1, planes)]
    back_planes = [lax.rem(plane + planes - f, planes) for f in range(1, planes)]
    fars = [{"row": 2 * p + parity} for p in far_planes]
    up, down = {"col": lax.rem(col + 1, n_col)}, {"col": lax.rem(col + n_col - 1, n_col)}
    has_up, has_down = col < n_col - 1, col > 0
    row_peers = [lax.rem(row + d, n_row) for d in range(1, n_row)]
    in_peers = [lax.rem(inner + e, n_in) for e in range(1, n_in)]
    home = lax.div(col, group)
    home_lane = pl.multiple_of(lax.rem(col, group) * cols, cols)
    total = 2 * slots * 0 + n_row * width

    meet(
        [{"row": r} for r in row_peers]
        + [{"col": lax.rem(col + d, n_col)} for d in range(1, n_col)]
        + [{"inner": p} for p in in_peers]
    )

    def at_rows(s):
        return pl.ds(pl.multiple_of(s * js, js), js)

    def x_at(s, k, p, q):
        return xg.at[k, at_rows(s), pl.ds(pl.multiple_of((2 * p + q) * width, width), width)]

    def v_at(s):
        return vg.at[:, :, pl.ds(pl.multiple_of(s * cols, cols), cols)]

    def z_at(s, p, q):
        return zt.at[s, pl.ds(pl.multiple_of((2 * p + q) * zrows, zrows), zrows)]

    def y_at(p, q):
        return yg.at[:, :, pl.ds(pl.multiple_of((2 * p + q) * width, width), width)]

    def x_line(s, k, way, src=None):
        place = x_at(s, k, plane, parity)
        return remote(
            place if src is None else src, place, x_z_send.at[way, s, k], x_z_recv.at[s, k], (up, down)[way]
        )

    def x_far(s, k, f, src=None):
        place = x_at(s, k, plane, parity)
        return remote(place if src is None else src, place, x_f_send.at[f, s, k], x_f_recv.at[f, s, k], fars[f])

    def x_twin(s, k, p, src=None):
        place = x_at(s, k, p, parity)
        return remote(place if src is None else src, place, x_t_send.at[p, s, k], x_t_recv.at[p, s, k], twin)

    def z_line(s, way, src=None):
        place = z_at(s, plane, parity)
        return remote(place if src is None else src, place, z_z_send.at[way, s], z_z_recv.at[s], (up, down)[way])

    def z_far(s, f, src=None):
        place = z_at(s, plane, parity)
        return remote(place if src is None else src, place, z_f_send.at[f, s], z_f_recv.at[f, s], fars[f])

    def z_twin(s, p, src=None):
        place = z_at(s, p, parity)
        return remote(place if src is None else src, place, z_t_send.at[p, s], z_t_recv.at[p, s], twin)

    def v_line(s, way, src=None):
        return remote(
            v_at(s) if src is None else src, v_at(s), v_send.at[way, s], v_recv.at[s], (up, down)[way]
        )

    def z_piece(d):
        rows = pl.ds(pl.multiple_of(row_peers[d] * zrows, zrows), zrows)
        return remote(zpart.at[rows], zgot.at[d], zp_send.at[d], zp_recv.at[d], {"row": row_peers[d]})

    def y_far(f):
        return remote(y_ref, y_at(plane, parity), y_f_send.at[f], y_f_recv.at[f], fars[f])

    def y_twin(p, src=None):
        place = y_at(p, parity)
        return remote(place if src is None else src, place, y_t_send.at[p], y_t_recv.at[p], twin)

    def s_peer(s, e):
        return remote(ssend.at[s], sgot.at[e, s], s_send.at[e, s], s_recv.at[e, s], {"inner": in_peers[e]})

    def m_home(s, source):
        return remote(msend.at[s], mgot.at[source], m_send.at[s], m_recv.at[source], {"col": s})

    def h_home(s, source):
        lane = pl.multiple_of(lax.rem(source, group) * cols, cols)
        return remote(
            hsend.at[s], s_home.at[:, pl.ds(lane, cols)], h_send.at[s], h_recv.at[lax.rem(source, group)], {"col": s}
        )

    def unit(b):
        both = jnp.minimum(col, n_col - 1 - col)
        near = lax.div(b + 1, 2)
        paired = jnp.where(lax.rem(b, 2) == 1, col - near, col + near)
        single = jnp.where(col < n_col - 1 - col, col + (b - both), col - (b - both))
        return jnp.where(b <= 2 * both, paired, single)

    fetches = [pltpu.make_async_copy(d_ref.at[k], deff.at[k], own.at[k]) for k in range(slots)]
    for fetch in fetches:
        fetch.start()

    @pl.when(has_up)
    def _():
        v_line(col, 0, v_ref).start()

    @pl.when(has_down)
    def _():
        v_line(col, 1, v_ref).start()

    for f in range(planes - 1):
        x_far(col, 0, f, x_ref.at[0]).start()
    for k in range(slots):
        x_twin(col, k, plane, x_ref.at[k]).start()
    y_twin(plane, y_ref).start()

    omega_at = pl.ds(pl.multiple_of(row * width, width), width)
    for j in range(own_j):
        inner_rows = jnp.concatenate([y_ref[k, j * rank : (j + 1) * rank] for k in range(slots)], axis=0)
        part = lax.dot_general(o_ref[j, :, omega_at], inner_rows, NT, preferred_element_type=WIDE)
        zpart[j * rank : (j + 1) * rank, 0:kr] = part
    for k in range(slots):
        xg[k, at_rows(col), pl.ds(pl.multiple_of(row * width, width), width)] = x_ref[k]
    vg[:, :, pl.ds(pl.multiple_of(col * cols, cols), cols)] = v_ref[...]
    yg[:, :, pl.ds(pl.multiple_of(row * width, width), width)] = y_ref[...]
    for d in range(n_row - 1):
        z_piece(d).start()
    for k in range(1, slots):
        for f in range(planes - 1):
            x_far(col, k, f, x_ref.at[k]).start()

    for t in range(1, n_col):

        @pl.when(col >= t)
        def _(t=t):
            v_line(col - t, 0).wait_recv()

            @pl.when(has_up)
            def _():
                v_line(col - t, 0).start()

        @pl.when(col + t < n_col)
        def _(t=t):
            v_line(col + t, 1).wait_recv()

            @pl.when(has_down)
            def _():
                v_line(col + t, 1).start()

    total_z = zpart[pl.ds(pl.multiple_of(row * zrows, zrows), zrows), 0:kr]
    for d in range(n_row - 1):
        z_piece(d).wait_recv()
        total_z = total_z + zgot[d, :, 0:kr]
    quarter = total_z.astype(NARROW)
    zown[:, 0:kr] = quarter
    zt[col, pl.ds(pl.multiple_of(row * zrows, zrows), zrows), 0:kr] = quarter

    @pl.when(has_up)
    def _():
        for k in range(slots):
            x_line(col, k, 0, x_ref.at[k]).start()
            if k == 0:
                z_line(col, 0, zown).start()

    @pl.when(has_down)
    def _():
        for k in range(slots):
            x_line(col, k, 1, x_ref.at[k]).start()
            if k == 0:
                z_line(col, 1, zown).start()

    for f in range(planes - 1):
        z_far(col, f, zown).start()
    z_twin(col, plane, zown).start()

    step_rows = min(512, total)
    for k in range(slots):
        fetches[k].wait()

        def effective(i, carry, k=k):
            at = pl.ds(pl.multiple_of(i * step_rows, step_rows), step_rows)
            low = lax.dot_general(vg[k, :, at], u_ref[k], TN, preferred_element_type=WIDE)
            dense = deff[k, at, :].astype(WIDE)
            deff[k, at, :] = jnp.where(mask_ref[k, 0:1, :] > 0.5, dense, low).astype(NARROW)
            return carry

        lax.fori_loop(0, total // step_rows, effective, 0)

    def pump(b, k):
        for side in range(2):
            s = col - (b + 1) if side == 0 else col + (b + 1)
            valid = s >= 0 if side == 0 else s < n_col

            @pl.when(valid)
            def _(s=s, side=side):
                x_line(s, k, side).wait_recv()

                @pl.when((has_up, has_down)[side])
                def _():
                    x_line(s, k, side).start()

                for f in range(planes - 1):
                    x_far(s, k, f).start()
                x_twin(s, k, plane).start()

                @pl.when(k == 0)
                def _():
                    z_line(s, side).wait_recv()

                    @pl.when((has_up, has_down)[side])
                    def _():
                        z_line(s, side).start()

                    for f in range(planes - 1):
                        z_far(s, f).start()
                    z_twin(s, plane).start()

        here = unit(b)
        for f in range(planes - 1):
            x_far(here, k, f).wait_recv()
            x_twin(here, k, back_planes[f]).start()

        @pl.when(k == 0)
        def _():
            for f in range(planes - 1):
                z_far(here, f).wait_recv()
                z_twin(here, back_planes[f]).start()

    def piece(b, k):
        s = unit(b)
        for p in range(planes):
            x_twin(s, k, p).wait_recv()
        out = jnp.dot(xg[k, at_rows(s), :], deff[k], preferred_element_type=WIDE).astype(NARROW)
        for j in range(own_j):
            pbuf[s, j, pl.ds(pl.multiple_of(k * rank, rank), rank), :] = out[j * rank : (j + 1) * rank]

    def sample(b):
        s = unit(b)
        for p in range(planes):
            z_twin(s, p).wait_recv()
        for j in range(own_j):
            rows = slice(j * rank, (j + 1) * rank)
            part = jnp.dot(zt[s, rows, 0:kr], pbuf[s, j], preferred_element_type=WIDE)
            spart[s, rows, :] = part
            ssend[s, rows, :] = part.astype(NARROW)
        for e in range(n_in - 1):
            s_peer(s, e).start()

    def finish(b):
        s = unit(b)
        for e in range(n_in - 1):
            s_peer(s, e).wait_recv()
        for j in range(own_j):
            rows = slice(j * rank, (j + 1) * rank)
            whole = spart[s, rows, :]
            for e in range(n_in - 1):
                whole = whole + sgot[e, s, rows, :].astype(WIDE)
            high, low = split(whole)
            hsend[s, rows, :] = high
            left = jnp.concatenate([high, low], axis=0)
            right = jnp.concatenate([pbuf[s, j], left], axis=0)
            both = lax.dot_general(left, right, NT, preferred_element_type=WIDE)
            top, low_part = both[:rank], both[rank:]
            cross = top[:, :kr] + low_part[:, :kr]
            gram = top[:, kr : kr + rank] + top[:, kr + rank :] + low_part[:, kr : kr + rank]
            gram_high, gram_low = split(gram)
            msend[s, rows, 0:kr] = cross.astype(NARROW)
            msend[s, rows, kr : kr + rank] = gram_high
            msend[s, rows, kr + rank : kr + 2 * rank] = gram_low

        @pl.when(s != col)
        def _():
            m_home(s, col).start()

            @pl.when(home == inner)
            def _():
                h_home(s, col).start()

        @pl.when(s == col)
        def _():
            mgot[col] = msend[s]

            @pl.when(home == inner)
            def _():
                s_home[:, pl.ds(home_lane, cols)] = hsend[s]

    count = n_col * slots

    def step(q, carry):
        @pl.when(q < count)
        def _():
            pump(lax.div(q, slots), lax.rem(q, slots))

        @pl.when(q == (n_col - 1) * slots)
        def _():
            for f in range(planes - 1):
                y_far(f).start()

        @pl.when(q > 0)
        def _():
            last = q - 1
            b, k = lax.div(last, slots), lax.rem(last, slots)
            piece(b, k)

            @pl.when(k == slots - 1)
            def _():
                sample(b)

                @pl.when(b > 0)
                def _():
                    finish(b - 1)

        return carry

    lax.fori_loop(0, count + 1, step, 0)
    finish(n_col - 1)

    for f in range(planes - 1):
        y_far(f).wait_recv()
        y_twin(back_planes[f]).start()
    for d in range(1, n_col):
        source = lax.rem(col + d, n_col)
        m_home(source, source).wait_recv()
    for g in range(group):
        source = inner * group + g

        @pl.when(source != col)
        def _(source=source):
            h_home(source, source).wait_recv()

    crosses = mgot[0, :, 0:kr].astype(WIDE)
    grams = mgot[0, :, kr : kr + rank].astype(WIDE) + mgot[0, :, kr + rank : kr + 2 * rank].astype(WIDE)
    for c in range(1, n_col):
        crosses = crosses + mgot[c, :, 0:kr].astype(WIDE)
        grams = grams + mgot[c, :, kr : kr + rank].astype(WIDE)
        grams = grams + mgot[c, :, kr + rank : kr + 2 * rank].astype(WIDE)
    cross_out[:, 0:kr] = crosses
    gram_out[...] = grams.reshape(own_j, rank, rank) * (1.0 / total)

    for p in range(planes):
        y_twin(p).wait_recv()
        y_twin(p).wait_send()
    for f in range(planes - 1):
        y_far(f).wait_send()
    for d in range(n_row - 1):
        z_piece(d).wait_send()

    def drain(s, carry):
        @pl.when(jnp.logical_and(has_up, s <= col))
        def _():
            v_line(s, 0).wait_send()
            z_line(s, 0).wait_send()
            for k in range(slots):
                x_line(s, k, 0).wait_send()

        @pl.when(jnp.logical_and(has_down, s >= col))
        def _():
            v_line(s, 1).wait_send()
            z_line(s, 1).wait_send()
            for k in range(slots):
                x_line(s, k, 1).wait_send()

        for f in range(planes - 1):
            z_far(s, f).wait_send()
            for k in range(slots):
                x_far(s, k, f).wait_send()
        for p in range(planes):
            z_twin(s, p).wait_send()
            for k in range(slots):
                x_twin(s, k, p).wait_send()
        for e in range(n_in - 1):
            s_peer(s, e).wait_send()

        @pl.when(s != col)
        def _():
            m_home(s, col).wait_send()

            @pl.when(home == inner)
            def _():
                h_home(s, col).wait_send()

        return carry

    lax.fori_loop(0, n_col, drain, 0)


def product(mask, u, v, d, x, y, omega, sizes):
    n_row, n_col, n_in = sizes
    slots, js, width = x.shape
    own_j, rank, total = omega.shape
    cols = u.shape[-1]
    planes = n_row // 2
    kr = slots * rank
    group = n_col // n_in
    share = total // n_in
    vmem = pl.BlockSpec(memory_space=pltpu.VMEM)
    dma = pltpu.SemaphoreType.DMA
    dims = (n_row, n_col, n_in, slots, own_j, rank, width, cols)
    return pl.pallas_call(
        functools.partial(product_kernel, dims),
        out_shape=(
            jax.ShapeDtypeStruct((js, share), NARROW),
            jax.ShapeDtypeStruct((js, lanes(kr)), WIDE),
            jax.ShapeDtypeStruct((own_j, rank, rank), WIDE),
            jax.ShapeDtypeStruct((slots, js, total), NARROW),
        ),
        in_specs=[vmem, vmem, vmem, pl.BlockSpec(memory_space=pltpu.HBM), vmem, vmem, vmem],
        out_specs=[vmem] * 4,
        scratch_shapes=[
            pltpu.VMEM((slots, n_col * js, total), NARROW),
            pltpu.VMEM((slots, rank, total), NARROW),
            pltpu.VMEM((slots, total, cols), NARROW),
            pltpu.VMEM((n_col, own_j, kr, cols), NARROW),
            pltpu.VMEM((n_col, js, lanes(kr)), NARROW),
            pltpu.VMEM((js, lanes(kr)), WIDE),
            pltpu.VMEM((n_row - 1, js // n_row, lanes(kr)), WIDE),
            pltpu.VMEM((js // n_row, lanes(kr)), NARROW),
            pltpu.VMEM((n_col, js, cols), WIDE),
            pltpu.VMEM((n_col, js, cols), NARROW),
            pltpu.VMEM((n_in - 1, n_col, js, cols), NARROW),
            pltpu.VMEM((n_col, js, lanes(kr + 2 * rank)), NARROW),
            pltpu.VMEM((n_col, js, lanes(kr + 2 * rank)), NARROW),
            pltpu.VMEM((n_col, js, cols), NARROW),
            dma((2, n_col, slots)), dma((n_col, slots)),
            dma((planes - 1, n_col, slots)), dma((planes - 1, n_col, slots)),
            dma((planes, n_col, slots)), dma((planes, n_col, slots)),
            dma((2, n_col)), dma((n_col,)),
            dma((2, n_col)), dma((n_col,)),
            dma((planes - 1, n_col)), dma((planes - 1, n_col)),
            dma((planes, n_col)), dma((planes, n_col)),
            dma((n_row - 1,)), dma((n_row - 1,)),
            dma((n_in - 1, n_col)), dma((n_in - 1, n_col)),
            dma((n_col,)), dma((n_col,)),
            dma((n_col,)), dma((group,)),
            dma((planes - 1,)), dma((planes - 1,)),
            dma((planes,)), dma((planes,)),
            dma((slots,)),
        ],
        compiler_params=pltpu.CompilerParams(
            collective_id=0, has_side_effects=True, vmem_limit_bytes=60 * 1024 * 1024
        ),
    )(mask, u, v, d, x, y, omega)


def factor_kernel(
    dims, s_ref, cross_ref, gram_ref, yg_ref, basis_ref, coupling_ref,
    inv, cross_got, yb, c_send, c_recv, y_send, y_recv, t_send, t_recv,
):
    n_in, slots, own_j, rank, share = dims
    half = own_j * rank // 2
    kr = slots * rank
    row, inner = lax.axis_index("row"), lax.axis_index("inner")
    parity = lax.rem(row, 2)
    twin = {"row": row + 1 - 2 * parity}
    peers = [lax.rem(inner + e, n_in) for e in range(1, n_in)]
    meet([twin] + [{"inner": peer} for peer in peers])
    mine = pl.ds(pl.multiple_of(parity * half, half), half)
    crosses, halves, passed = [], [], []
    for e, peer in enumerate(peers):
        there = {"inner": peer}
        lane = pl.ds(pl.multiple_of(peer * share, share), share)
        crosses.append(remote(cross_ref, cross_got.at[e], c_send.at[e], c_recv.at[e], there))
        halves.append(
            remote(yg_ref.at[:, mine, lane], yb.at[e, :, mine], y_send.at[e], y_recv.at[e], there)
        )
        passed.append(remote(yb.at[e, :, mine], yb.at[e, :, mine], t_send.at[e], t_recv.at[e], twin))
    for copy in crosses + halves:
        copy.start()
    inverse_factor(gram_ref[...], inv)
    for e in range(n_in - 1):
        halves[e].wait_recv()
        passed[e].start()
    for copy in crosses:
        copy.wait()
    scale = 1.0 / math.sqrt(share * n_in)
    lane = pl.ds(pl.multiple_of(inner * share, share), share)
    left = []
    for j in range(own_j):
        rows = slice(j * rank, (j + 1) * rank)
        high, low = split(inv[j])
        both = jnp.concatenate([high, low], axis=0)
        out = jnp.dot(both, s_ref[rows, :], preferred_element_type=WIDE)
        basis_ref[j] = out[:rank] + out[rank:]
        crossed = jnp.concatenate(
            [cross_ref[rows, 0:kr]] + [cross_got[e, rows, 0:kr] for e in range(n_in - 1)], axis=1
        )
        projected = jnp.dot(inv[j], crossed, precision=HIGHEST, preferred_element_type=WIDE) * scale
        left.append(jnp.concatenate(split(projected), axis=0))
    for copy in passed:
        copy.wait_recv()
    for j in range(own_j):
        rows = slice(j * rank, (j + 1) * rank)
        right = [yg_ref[k, rows, lane] for k in range(slots)]
        right += [yb[e, k, rows, :] for e in range(n_in - 1) for k in range(slots)]
        out = jnp.dot(left[j], jnp.concatenate(right, axis=0), preferred_element_type=WIDE)
        coupling_ref[j] = out[:rank] + out[rank:]
    for copy in halves + passed:
        copy.wait_send()


def factor(s_home, cross, gram, yg, n_in):
    slots, js, total = yg.shape
    own_j, rank, _ = gram.shape
    share = total // n_in
    vmem = pl.BlockSpec(memory_space=pltpu.VMEM)
    dma = pltpu.SemaphoreType.DMA((n_in - 1,))
    out = jax.ShapeDtypeStruct((own_j, rank, share), WIDE)
    return pl.pallas_call(
        functools.partial(factor_kernel, (n_in, slots, own_j, rank, share)),
        out_shape=(out, out),
        in_specs=[vmem] * 4,
        out_specs=[vmem] * 2,
        scratch_shapes=[
            pltpu.VMEM(gram.shape, WIDE),
            pltpu.VMEM((n_in - 1,) + cross.shape, WIDE),
            pltpu.VMEM((n_in - 1, slots, js, share), NARROW),
        ] + [dma] * 6,
        compiler_params=pltpu.CompilerParams(collective_id=1, has_side_effects=True),
    )(s_home, cross, gram, yg)


def inverse_factor(gram, out_ref):
    count, size, _ = gram.shape
    tall = lax.broadcasted_iota(jnp.int32, (size, size), 0)
    wide = lax.broadcasted_iota(jnp.int32, (size, size), 1)
    eye = (tall == wide).astype(WIDE)
    lines = lax.broadcasted_iota(jnp.int32, (8, 1), 0)
    works = []
    for j in range(count):
        full = jnp.concatenate([gram[j], eye], axis=1)
        works.append([full[8 * b : 8 * b + 8] for b in range(size // 8)])
    scales = [[] for _ in range(count)]
    for k in range(size):
        b0, in_b = k // 8, k % 8
        for j in range(count):
            work = works[j]
            line = work[b0][in_b : in_b + 1]
            pivot = line[:, k : k + 1]
            scales[j].append(lax.rsqrt(pivot))
            line = line * (1.0 / pivot)
            for b in range(b0, size // 8):
                column = work[b][:, k : k + 1]
                if b == b0:
                    if in_b == 7:
                        continue
                    column = jnp.where(lines > in_b, column, 0.0)
                work[b] = work[b] - column * line
    for j in range(count):
        scale = jnp.concatenate(scales[j], axis=0)
        out_ref[j] = jnp.concatenate(works[j], axis=0)[:, size:] * scale


def local(sizes, near_flags, row_factor, col_factor, near_block, inner_left, inner_right, sketch_matrix):
    slots, own_j, rank, width = inner_left.shape
    js = own_j * rank
    cols = row_factor.shape[-1]
    mask = jnp.broadcast_to(near_flags[0].astype(WIDE)[:, None, None], (slots, 8, cols))
    s_home, cross, gram, yg = product(
        mask, row_factor[0], col_factor[0], near_block[0],
        inner_left.reshape(slots, js, width), inner_right.reshape(slots, js, width), sketch_matrix, sizes,
    )
    basis, coupling = factor(s_home, cross, gram, yg, sizes[2])
    return (basis[None], coupling[None])


def solution(mesh):
    sizes = (mesh.shape["row"], mesh.shape["col"], mesh.shape["inner"])
    in_specs = (
        P("row", "inner"),
        P("row", "inner", None, "col"),
        P("row", "inner", None, "col"),
        P("row", "inner", None, "col"),
        P("inner", "col", None, "row"),
        P("inner", "col", None, "row"),
        P("col", None, None),
    )
    out_specs = (P("row", "col", None, "inner"), P("row", "col", None, "inner"))
    return jax.shard_map(
        functools.partial(local, sizes), mesh=mesh, in_specs=in_specs, out_specs=out_specs, check_vma=False
    )
```

```python
import functools
import math

import jax
import jax.numpy as jnp
from jax import lax
from jax.experimental import pallas as pl
from jax.experimental.pallas import tpu as pltpu
from jax.sharding import PartitionSpec as P

MESH = pl.DeviceIdType.MESH
HIGHEST = lax.Precision.HIGHEST
WIDE = jnp.float32
NARROW = jnp.bfloat16
NT = (((1,), (1,)), ((), ()))
TN = (((0,), (0,)), ((), ()))


def remote(src, dst, send, recv, device):
    return pltpu.make_async_remote_copy(
        src_ref=src, dst_ref=dst, send_sem=send, recv_sem=recv, device_id=device, device_id_type=MESH
    )


def meet(devices):
    barrier = pltpu.get_barrier_semaphore()
    for device in devices:
        pl.semaphore_signal(barrier, inc=1, device_id=device, device_id_type=MESH)
    pl.semaphore_wait(barrier, len(devices))


def split(value):
    high = value.astype(NARROW)
    return high, (value - high.astype(WIDE)).astype(NARROW)


def lanes(length):
    return -(-length // 128) * 128


def product_kernel(
    dims, flag_ref, u_ref, v_ref, d_ref, x_ref, y_ref, o_ref,
    basis_ref, coupling_ref,
    xg, vg, yg, yb, deff, pbuf, zt, zpart, zgot, zown, spart, ssend, sgot, msend, mgot, hsend, hrel, s_home,
    cross_sum, cross_got, inv,
    x_z_send, x_z_recv, x_f_send, x_f_recv, x_t_send, x_t_recv,
    v_send, v_recv, z_z_send, z_z_recv, z_f_send, z_f_recv, z_t_send, z_t_recv, zp_send, zp_recv,
    s_send, s_recv, m_send, m_recv, h_send, h_recv, r_send, r_recv, f_send, f_recv,
    y_f_send, y_f_recv, y_t_send, y_t_recv, y_y_send, y_y_recv, y_p_send, y_p_recv, c_send, c_recv, own,
):
    n_row, n_col, n_in, slots, own_j, rank, width, cols = dims
    js = own_j * rank
    half = js // 2
    kr = slots * rank
    total = n_row * width
    share = total // n_in
    group = n_col // n_in
    planes = n_row // 2
    zrows = js // n_row
    row, col, inner = lax.axis_index("row"), lax.axis_index("col"), lax.axis_index("inner")
    plane = lax.div(row, 2)
    parity = lax.rem(row, 2)
    twin = {"row": row + 1 - 2 * parity}
    far_planes = [lax.rem(plane + f, planes) for f in range(1, planes)]
    back_planes = [lax.rem(plane + planes - f, planes) for f in range(1, planes)]
    fars = [{"row": 2 * p + parity} for p in far_planes]
    up, down = {"col": lax.rem(col + 1, n_col)}, {"col": lax.rem(col + n_col - 1, n_col)}
    has = (col < n_col - 1, col > 0)
    row_peers = [lax.rem(row + d, n_row) for d in range(1, n_row)]
    in_peers = [lax.rem(inner + e, n_in) for e in range(1, n_in)]
    home = lax.div(col, group)
    helper = lax.rem(home + 1, n_in)
    helped = lax.rem(inner + n_in - 1, n_in)
    mine = pl.ds(pl.multiple_of(parity * half, half), half)

    fetches = [pltpu.make_async_copy(d_ref.at[k], deff.at[k], own.at[k]) for k in range(slots)]
    for fetch in fetches:
        fetch.start()

    meet(
        [{"row": r} for r in row_peers]
        + [{"col": lax.rem(col + d, n_col)} for d in range(1, n_col)]
        + [{"inner": p} for p in in_peers]
    )

    def at_rows(s):
        return pl.ds(pl.multiple_of(s * js, js), js)

    def x_at(s, k, p, q):
        return xg.at[k, at_rows(s), pl.ds(pl.multiple_of((2 * p + q) * width, width), width)]

    def v_at(s):
        return vg.at[:, :, pl.ds(pl.multiple_of(s * cols, cols), cols)]

    def z_at(s, p, q):
        return zt.at[s, pl.ds(pl.multiple_of((2 * p + q) * zrows, zrows), zrows)]

    def y_at(p, q):
        return yg.at[:, :, pl.ds(pl.multiple_of((2 * p + q) * width, width), width)]

    def x_line(s, k, way, src=None):
        place = x_at(s, k, plane, parity)
        return remote(
            place if src is None else src, place, x_z_send.at[way, s, k], x_z_recv.at[s, k], (up, down)[way]
        )

    def x_far(s, k, f, src=None):
        place = x_at(s, k, plane, parity)
        return remote(place if src is None else src, place, x_f_send.at[f, s, k], x_f_recv.at[f, s, k], fars[f])

    def x_twin(s, k, p, src=None):
        place = x_at(s, k, p, parity)
        return remote(place if src is None else src, place, x_t_send.at[p, s, k], x_t_recv.at[p, s, k], twin)

    def z_line(s, way, src=None):
        place = z_at(s, plane, parity)
        return remote(place if src is None else src, place, z_z_send.at[way, s], z_z_recv.at[s], (up, down)[way])

    def z_far(s, f, src=None):
        place = z_at(s, plane, parity)
        return remote(place if src is None else src, place, z_f_send.at[f, s], z_f_recv.at[f, s], fars[f])

    def z_twin(s, p, src=None):
        place = z_at(s, p, parity)
        return remote(place if src is None else src, place, z_t_send.at[p, s], z_t_recv.at[p, s], twin)

    def v_line(s, way, src=None):
        return remote(
            v_at(s) if src is None else src, v_at(s), v_send.at[way, s], v_recv.at[s], (up, down)[way]
        )

    def z_piece(d):
        rows = pl.ds(pl.multiple_of(row_peers[d] * zrows, zrows), zrows)
        return remote(zpart.at[rows], zgot.at[d], zp_send.at[d], zp_recv.at[d], {"row": row_peers[d]})

    def y_far(f):
        return remote(y_ref, y_at(plane, parity), y_f_send.at[f], y_f_recv.at[f], fars[f])

    def y_twin(p, src=None):
        place = y_at(p, parity)
        return remote(place if src is None else src, place, y_t_send.at[p], y_t_recv.at[p], twin)

    def y_inner(e):
        lane = pl.ds(pl.multiple_of(in_peers[e] * share, share), share)
        return remote(
            yg.at[:, mine, lane], yb.at[e, :, mine], y_y_send.at[e], y_y_recv.at[e], {"inner": in_peers[e]}
        )

    def y_pass(e):
        return remote(yb.at[e, :, mine], yb.at[e, :, mine], y_p_send.at[e], y_p_recv.at[e], twin)

    def share_plane(peer):
        return lax.div(peer * share, 2 * width)

    def s_peer(s, h, e):
        rows = pl.ds(h * half, half)
        return remote(
            ssend.at[s, rows], sgot.at[e, s, rows], s_send.at[e, s, h], s_recv.at[e, s, h], {"inner": in_peers[e]}
        )

    def m_home(s, h, source):
        return remote(msend.at[s, h], mgot.at[source, h], m_send.at[s, h], m_recv.at[source, h], {"col": s})

    def home_at(g, h):
        return s_home.at[pl.ds(h * half, half), pl.ds(pl.multiple_of(g * cols, cols), cols)]

    def h_home(s, g):
        return remote(hsend.at[s, pl.ds(0, half)], home_at(g, 0), h_send.at[s], h_recv.at[g], {"col": s})

    def h_relay(s, g):
        return remote(hsend.at[s, pl.ds(half, half)], hrel.at[g], r_send.at[s], r_recv.at[g], {"col": s})

    def h_pass(g, src=None):
        return remote(
            hrel.at[g] if src is None else src, home_at(g, 1), f_send.at[g], f_recv.at[g], {"inner": helped}
        )

    def c_inner(e):
        return remote(cross_sum, cross_got.at[e], c_send.at[e], c_recv.at[e], {"inner": in_peers[e]})

    def unit(b):
        both = jnp.minimum(col, n_col - 1 - col)
        near = lax.div(b + 1, 2)
        paired = jnp.where(lax.rem(b, 2) == 1, col - near, col + near)
        single = jnp.where(col < n_col - 1 - col, col + (b - both), col - (b - both))
        return jnp.where(b <= 2 * both, paired, single)

    def own_line(k):
        for way in range(2):

            @pl.when(has[way])
            def _(way=way):
                x_line(col, k, way, x_ref.at[k]).start()

    for way in range(2):

        @pl.when(has[way])
        def _(way=way):
            v_line(col, way, v_ref).start()

    own_line(0)
    for f in range(planes - 1):
        x_far(col, 0, f, x_ref.at[0]).start()
    y_twin(plane, y_ref).start()
    for k in range(slots):
        x_twin(col, k, plane, x_ref.at[k]).start()

    omega_at = pl.ds(pl.multiple_of(row * width, width), width)
    for j in range(own_j):
        inner_rows = jnp.concatenate([y_ref[k, j * rank : (j + 1) * rank] for k in range(slots)], axis=0)
        part = lax.dot_general(o_ref[j, :, omega_at], inner_rows, NT, preferred_element_type=WIDE)
        zpart[j * rank : (j + 1) * rank, 0:kr] = part
    for k in range(slots):
        xg[k, at_rows(col), pl.ds(pl.multiple_of(row * width, width), width)] = x_ref[k]
    vg[:, :, pl.ds(pl.multiple_of(col * cols, cols), cols)] = v_ref[...]
    yg[:, :, pl.ds(pl.multiple_of(row * width, width), width)] = y_ref[...]
    for d in range(n_row - 1):
        z_piece(d).start()
    for k in range(1, slots):
        for f in range(planes - 1):
            x_far(col, k, f, x_ref.at[k]).start()
    y_twin(plane).wait_recv()
    for e in range(n_in - 1):

        @pl.when(share_plane(in_peers[e]) == plane)
        def _(e=e):
            y_inner(e).start()

    def gather_z():
        total_z = zpart[pl.ds(pl.multiple_of(row * zrows, zrows), zrows), 0:kr]
        for d in range(n_row - 1):
            z_piece(d).wait_recv()
            total_z = total_z + zgot[d, :, 0:kr]
        quarter = total_z.astype(NARROW)
        zown[:, 0:kr] = quarter
        zt[col, pl.ds(pl.multiple_of(row * zrows, zrows), zrows), 0:kr] = quarter
        for way in range(2):

            @pl.when(has[way])
            def _(way=way):
                z_line(col, way, zown).start()

        for f in range(planes - 1):
            z_far(col, f, zown).start()
        z_twin(col, plane, zown).start()

    def along(t, act):
        for way in range(2):
            s = col - t if way == 0 else col + t

            @pl.when(s >= 0 if way == 0 else s < n_col)
            def _(s=s, way=way):
                act(s, way)

    def pass_v(s, way):
        v_line(s, way).wait_recv()

        @pl.when(has[way])
        def _():
            v_line(s, way).start()

    def pass_z(s, way):
        z_line(s, way).wait_recv()

        @pl.when(has[way])
        def _():
            z_line(s, way).start()

        z_twin(s, plane).start()

    def pump(b, k):
        def pass_x(s, way):
            x_line(s, k, way).wait_recv()

            @pl.when(has[way])
            def _():
                x_line(s, k, way).start()

            x_twin(s, k, plane).start()

        along(b + 1, pass_x)

        @pl.when(b + 1 < n_col)
        def _():
            ahead = unit(b + 1)
            for f in range(planes - 1):
                x_far(ahead, k, f).start()

        here = unit(b)

        @pl.when(jnp.logical_and(k == 0, b > 0))
        def _():
            along(b, pass_z)
            for f in range(planes - 1):
                z_far(here, f).start()

        for f in range(planes - 1):
            x_far(here, k, f).wait_recv()
            x_twin(here, k, back_planes[f]).start()

        @pl.when(k == slots - 1)
        def _():
            for f in range(planes - 1):
                z_far(here, f).wait_recv()
                z_twin(here, back_planes[f]).start()

    step_rows = min(512, total)

    def effective(k):
        pltpu.make_async_copy(d_ref.at[k], deff.at[k], own.at[k]).wait()
        near = jnp.full((1, cols), flag_ref[0, k], jnp.int32) > 0

        def some(i, carry):
            at = pl.ds(pl.multiple_of(i * step_rows, step_rows), step_rows)
            low = lax.dot_general(vg[k, :, at], u_ref[k], TN, preferred_element_type=WIDE)
            dense = deff[k, at, :].astype(WIDE)
            deff[k, at, :] = jnp.where(near, dense, low).astype(NARROW)
            return carry

        lax.fori_loop(0, total // step_rows, some, 0)

    def piece(b, k):
        @pl.when(b == 0)
        def _():
            effective(k)

        s = unit(b)
        for p in range(planes):
            x_twin(s, k, p).wait_recv()
        out = jnp.dot(xg[k, at_rows(s), :], deff[k], preferred_element_type=WIDE).astype(NARROW)
        for j in range(own_j):
            pbuf[s, j, pl.ds(pl.multiple_of(k * rank, rank), rank), :] = out[j * rank : (j + 1) * rank]

    def sample(b):
        s = unit(b)
        for p in range(planes):
            z_twin(s, p).wait_recv()
        for h in range(2):
            for j in range(h * own_j // 2, (h + 1) * own_j // 2):
                rows = slice(j * rank, (j + 1) * rank)
                part = jnp.dot(zt[s, rows, 0:kr], pbuf[s, j], preferred_element_type=WIDE)
                spart[s, rows, :] = part
                ssend[s, rows, :] = part.astype(NARROW)
            for e in range(n_in - 1):
                s_peer(s, h, e).start()

    def finish(b):
        s = unit(b)
        away = s != col
        lane = lax.rem(col, group)
        for h in range(2):
            for e in range(n_in - 1):
                s_peer(s, h, e).wait_recv()
            lows = []
            for i in range(own_j // 2):
                j = h * (own_j // 2) + i
                rows = slice(j * rank, (j + 1) * rank)
                whole = spart[s, rows, :]
                for e in range(n_in - 1):
                    whole = whole + sgot[e, s, rows, :].astype(WIDE)
                high, low = split(whole)
                hsend[s, rows, :] = high
                left = jnp.concatenate([high, low], axis=0)
                right = jnp.concatenate([pbuf[s, j], left], axis=0)
                both = lax.dot_general(left, right, NT, preferred_element_type=WIDE)
                top, under = both[:rank], both[rank:]
                cross = top[:, :kr] + under[:, :kr]
                gram = top[:, kr : kr + rank] + top[:, kr + rank :] + under[:, kr : kr + rank]
                gram_high, gram_low = split(gram)
                at = slice(i * rank, (i + 1) * rank)
                msend[s, h, at, 0:kr] = cross.astype(NARROW)
                msend[s, h, at, kr : kr + rank] = gram_high
                lows.append(gram_low)
            pair = jnp.concatenate(lows, axis=1)
            folds = (kr + rank) // pair.shape[1]
            deep = rank // folds
            msend[s, h, half : half + deep] = jnp.concatenate(
                [pair[i * deep : (i + 1) * deep] for i in range(folds)], axis=1
            )

            @pl.when(away)
            def _(h=h):
                m_home(s, h, col).start()

            if h == 0:

                @pl.when(jnp.logical_and(away, home == inner))
                def _():
                    h_home(s, lane).start()

            else:

                @pl.when(jnp.logical_and(away, helper == inner))
                def _():
                    h_relay(s, lane).start()

        @pl.when(jnp.logical_not(away))
        def _():
            mgot[col] = msend[s]

            @pl.when(home == inner)
            def _():
                s_home[0:half, pl.ds(pl.multiple_of(lane * cols, cols), cols)] = hsend[s, 0:half]

    count = n_col * slots
    ready = n_col - 2

    def done(q):
        return jnp.maximum(jnp.minimum(q, 2 * (q - ready + 1)), 0)

    def work(i, carry):
        b, k = lax.div(i, slots), lax.rem(i, slots)
        piece(b, k)

        @pl.when(k == slots - 1)
        def _():
            sample(b)

        @pl.when(jnp.logical_and(k == min(1, slots - 1), b > 0))
        def _():
            finish(b - 1)

        return carry

    def step(q, carry):
        @pl.when(q < n_col - 1)
        def _():
            along(q + 1, pass_v)

        @pl.when(q + 1 < slots)
        def _():
            own_line(q + 1)

        @pl.when(q < count)
        def _():
            pump(lax.div(q, slots), lax.rem(q, slots))

        @pl.when(q == 0)
        def _():
            gather_z()

        @pl.when(q == (n_col - 1) * slots)
        def _():
            for f in range(planes - 1):
                y_far(f).start()

        lax.fori_loop(done(q - 1), done(q), work, 0)
        return carry

    lax.fori_loop(0, count + 1, step, 0)
    finish(n_col - 1)

    for f in range(planes - 1):
        y_far(f).wait_recv()
        y_twin(back_planes[f]).start()
    for g in range(group):
        source = helped * group + g

        @pl.when(source != col)
        def _(g=g, source=source):
            h_relay(source, g).wait_recv()
            h_pass(g).start()

        @pl.when(source == col)
        def _(g=g):
            h_pass(g, hsend.at[col, pl.ds(half, half)]).start()

    for f in range(planes - 1):
        y_twin(back_planes[f]).wait_recv()
    for e in range(n_in - 1):

        @pl.when(share_plane(in_peers[e]) != plane)
        def _(e=e):
            y_inner(e).start()

    for d in range(1, n_col):
        source = lax.rem(col + d, n_col)
        for h in range(2):
            m_home(source, h, source).wait_recv()
    grams = []
    for h in range(2):
        crosses = mgot[0, h, 0:half, 0:kr].astype(WIDE)
        high = mgot[0, h, 0:half, kr : kr + rank].astype(WIDE)
        deep = msend.shape[2] - half
        under = mgot[0, h, half : half + deep].astype(WIDE)
        for c in range(1, n_col):
            crosses = crosses + mgot[c, h, 0:half, 0:kr].astype(WIDE)
            high = high + mgot[c, h, 0:half, kr : kr + rank].astype(WIDE)
            under = under + mgot[c, h, half : half + deep].astype(WIDE)
        cross_sum[h * half : (h + 1) * half, 0:kr] = crosses
        wide = half
        pair = jnp.concatenate([under[:, i * wide : (i + 1) * wide] for i in range(under.shape[1] // wide)], axis=0)
        for i in range(own_j // 2):
            grams.append(high[i * rank : (i + 1) * rank] + pair[:, i * rank : (i + 1) * rank])
    for e in range(n_in - 1):
        c_inner(e).start()
    inverse_factor(grams, inv)

    for g in range(group):
        source = inner * group + g

        @pl.when(source != col)
        def _(g=g, source=source):
            h_home(source, g).wait_recv()

        h_pass(g).wait_recv()
    for e in range(n_in - 1):
        y_inner(e).wait_recv()
        y_pass(e).start()
    for j in range(own_j):
        rows = slice(j * rank, (j + 1) * rank)
        both = jnp.concatenate(split(inv[j]), axis=0)
        out = jnp.dot(both, s_home[rows, :], preferred_element_type=WIDE)
        basis_ref[j] = out[:rank] + out[rank:]
    for e in range(n_in - 1):
        c_inner(e).wait_recv()
    left = []
    for j in range(own_j):
        rows = slice(j * rank, (j + 1) * rank)
        crossed = jnp.concatenate(
            [cross_sum[rows, 0:kr]] + [cross_got[e, rows, 0:kr] for e in range(n_in - 1)], axis=1
        )
        projected = jnp.dot(inv[j], crossed, precision=HIGHEST, preferred_element_type=WIDE)
        left.append(jnp.concatenate(split(projected), axis=0))
    for e in range(n_in - 1):
        y_pass(e).wait_recv()
    lane_own = pl.ds(pl.multiple_of(inner * share, share), share)
    for j in range(own_j):
        rows = slice(j * rank, (j + 1) * rank)
        right = [yg[k, rows, lane_own] for k in range(slots)]
        right += [yb[e, k, rows, :] for e in range(n_in - 1) for k in range(slots)]
        out = jnp.dot(left[j], jnp.concatenate(right, axis=0), preferred_element_type=WIDE)
        coupling_ref[j] = out[:rank] + out[rank:]

    for p in range(planes):
        y_twin(p).wait_send()
    for f in range(planes - 1):
        y_far(f).wait_send()
    for d in range(n_row - 1):
        z_piece(d).wait_send()
    for e in range(n_in - 1):
        y_inner(e).wait_send()
        y_pass(e).wait_send()
        c_inner(e).wait_send()
    for g in range(group):
        h_pass(g).wait_send()

    def drain(s, carry):
        for way in range(2):

            @pl.when(jnp.logical_and(has[way], s <= col if way == 0 else s >= col))
            def _(way=way):
                v_line(s, way).wait_send()
                z_line(s, way).wait_send()
                for k in range(slots):
                    x_line(s, k, way).wait_send()

        for f in range(planes - 1):
            z_far(s, f).wait_send()
            for k in range(slots):
                x_far(s, k, f).wait_send()
        for p in range(planes):
            z_twin(s, p).wait_send()
            for k in range(slots):
                x_twin(s, k, p).wait_send()
        for e in range(n_in - 1):
            for h in range(2):
                s_peer(s, h, e).wait_send()

        @pl.when(s != col)
        def _():
            for h in range(2):
                m_home(s, h, col).wait_send()

            @pl.when(home == inner)
            def _():
                h_home(s, 0).wait_send()

            @pl.when(helper == inner)
            def _():
                h_relay(s, 0).wait_send()

        return carry

    lax.fori_loop(0, n_col, drain, 0)


def product(flags, u, v, d, x, y, omega, sizes):
    n_row, n_col, n_in = sizes
    slots, js, width = x.shape
    own_j, rank, total = omega.shape
    cols = u.shape[-1]
    planes = n_row // 2
    kr = slots * rank
    group = n_col // n_in
    share = total // n_in
    half = js // 2
    packed = half + rank * (own_j // 2) * rank // (kr + rank)
    vmem = pl.BlockSpec(memory_space=pltpu.VMEM)
    dma = pltpu.SemaphoreType.DMA
    dims = (n_row, n_col, n_in, slots, own_j, rank, width, cols)
    out = jax.ShapeDtypeStruct((own_j, rank, share), WIDE)
    return pl.pallas_call(
        functools.partial(product_kernel, dims),
        out_shape=(out, out),
        in_specs=[
            pl.BlockSpec(memory_space=pltpu.SMEM), vmem, vmem, pl.BlockSpec(memory_space=pltpu.HBM), vmem, vmem, vmem
        ],
        out_specs=[vmem] * 2,
        scratch_shapes=[
            pltpu.VMEM((slots, n_col * js, total), NARROW),
            pltpu.VMEM((slots, rank, total), NARROW),
            pltpu.VMEM((slots, js, total), NARROW),
            pltpu.VMEM((n_in - 1, slots, js, share), NARROW),
            pltpu.VMEM((slots, total, cols), NARROW),
            pltpu.VMEM((n_col, own_j, kr, cols), NARROW),
            pltpu.VMEM((n_col, js, lanes(kr)), NARROW),
            pltpu.VMEM((js, lanes(kr)), WIDE),
            pltpu.VMEM((n_row - 1, js // n_row, lanes(kr)), WIDE),
            pltpu.VMEM((js // n_row, lanes(kr)), NARROW),
            pltpu.VMEM((n_col, js, cols), WIDE),
            pltpu.VMEM((n_col, js, cols), NARROW),
            pltpu.VMEM((n_in - 1, n_col, js, cols), NARROW),
            pltpu.VMEM((n_col, 2, packed, kr + rank), NARROW),
            pltpu.VMEM((n_col, 2, packed, kr + rank), NARROW),
            pltpu.VMEM((n_col, js, cols), NARROW),
            pltpu.VMEM((group, half, cols), NARROW),
            pltpu.VMEM((js, share), NARROW),
            pltpu.VMEM((js, lanes(kr)), WIDE),
            pltpu.VMEM((n_in - 1, js, lanes(kr)), WIDE),
            pltpu.VMEM((own_j, rank, rank), WIDE),
            dma((2, n_col, slots)), dma((n_col, slots)),
            dma((planes - 1, n_col, slots)), dma((planes - 1, n_col, slots)),
            dma((planes, n_col, slots)), dma((planes, n_col, slots)),
            dma((2, n_col)), dma((n_col,)),
            dma((2, n_col)), dma((n_col,)),
            dma((planes - 1, n_col)), dma((planes - 1, n_col)),
            dma((planes, n_col)), dma((planes, n_col)),
            dma((n_row - 1,)), dma((n_row - 1,)),
            dma((n_in - 1, n_col, 2)), dma((n_in - 1, n_col, 2)),
            dma((n_col, 2)), dma((n_col, 2)),
            dma((n_col,)), dma((group,)),
            dma((n_col,)), dma((group,)),
            dma((group,)), dma((group,)),
            dma((planes - 1,)), dma((planes - 1,)),
            dma((planes,)), dma((planes,)),
            dma((n_in - 1,)), dma((n_in - 1,)),
            dma((n_in - 1,)), dma((n_in - 1,)),
            dma((n_in - 1,)), dma((n_in - 1,)),
            dma((slots,)),
        ],
        compiler_params=pltpu.CompilerParams(
            collective_id=0, has_side_effects=True, vmem_limit_bytes=60 * 1024 * 1024
        ),
    )(flags, u, v, d, x, y, omega)


def inverse_factor(gram, out_ref):
    count, size = len(gram), gram[0].shape[0]
    tall = lax.broadcasted_iota(jnp.int32, (size, size), 0)
    wide = lax.broadcasted_iota(jnp.int32, (size, size), 1)
    eye = (tall == wide).astype(WIDE)
    lines = lax.broadcasted_iota(jnp.int32, (8, 1), 0)
    works = []
    for j in range(count):
        full = jnp.concatenate([gram[j], eye], axis=1)
        works.append([full[8 * b : 8 * b + 8] for b in range(size // 8)])
    scales = [[] for _ in range(count)]
    for k in range(size):
        b0, in_b = k // 8, k % 8
        for j in range(count):
            work = works[j]
            line = work[b0][in_b : in_b + 1]
            pivot = line[:, k : k + 1]
            scales[j].append(lax.rsqrt(pivot))
            line = line * (1.0 / pivot)
            for b in range(b0, size // 8):
                column = work[b][:, k : k + 1]
                if b == b0:
                    if in_b == 7:
                        continue
                    column = jnp.where(lines > in_b, column, 0.0)
                work[b] = work[b] - column * line
    for j in range(count):
        scale = jnp.concatenate(scales[j], axis=0)
        out_ref[j] = jnp.concatenate(works[j], axis=0)[:, size:] * scale


def local(sizes, near_flags, row_factor, col_factor, near_block, inner_left, inner_right, sketch_matrix):
    slots, own_j, rank, width = inner_left.shape
    js = own_j * rank
    basis, coupling = product(
        near_flags, row_factor[0], col_factor[0], near_block[0],
        inner_left.reshape(slots, js, width), inner_right.reshape(slots, js, width), sketch_matrix, sizes,
    )
    return (basis[None] * math.sqrt(width * sizes[0]), coupling[None])


def solution(mesh):
    sizes = (mesh.shape["row"], mesh.shape["col"], mesh.shape["inner"])
    in_specs = (
        P("row", "inner"),
        P("row", "inner", None, "col"),
        P("row", "inner", None, "col"),
        P("row", "inner", None, "col"),
        P("inner", "col", None, "row"),
        P("inner", "col", None, "row"),
        P("col", None, None),
    )
    out_specs = (P("row", "col", None, "inner"), P("row", "col", None, "inner"))
    return jax.shard_map(
        functools.partial(local, sizes), mesh=mesh, in_specs=in_specs, out_specs=out_specs, check_vma=False
    )
```

```python
import functools
import math

import jax
import jax.numpy as jnp
from jax import lax
from jax.experimental import pallas as pl
from jax.experimental.pallas import tpu as pltpu
from jax.sharding import PartitionSpec as P

MESH = pl.DeviceIdType.MESH
HIGHEST = lax.Precision.HIGHEST
WIDE = jnp.float32
NARROW = jnp.bfloat16
NT = (((1,), (1,)), ((), ()))
TN = (((0,), (0,)), ((), ()))


def remote(src, dst, send, recv, device):
    return pltpu.make_async_remote_copy(
        src_ref=src, dst_ref=dst, send_sem=send, recv_sem=recv, device_id=device, device_id_type=MESH
    )


def meet(devices):
    barrier = pltpu.get_barrier_semaphore()
    for device in devices:
        pl.semaphore_signal(barrier, inc=1, device_id=device, device_id_type=MESH)
    pl.semaphore_wait(barrier, len(devices))


def split(value):
    high = value.astype(NARROW)
    return high, (value - high.astype(WIDE)).astype(NARROW)


def lanes(length):
    return -(-length // 128) * 128


def product_kernel(
    dims, flag_ref, u_hbm, v_hbm, d_ref, x_hbm, y_hbm, o_hbm,
    basis_ref, coupling_ref,
    u_ref, o_ref,
    xg, vg, yg, yb, deff, pbuf, zt, zpart, zgot, zown, spart, ssend, sgot, msend, mgot, hsend, hrel, s_home,
    cross_sum, cross_pass, cross_got, inv,
    x_z_send, x_z_recv, x_f_send, x_f_recv, x_t_send, x_t_recv, x_s_send, x_s_recv,
    v_send, v_recv, z_z_send, z_z_recv, z_f_send, z_f_recv, z_t_send, z_t_recv, zp_send, zp_recv,
    s_send, s_recv, m_send, m_recv, h_send, h_recv, r_send, r_recv, f_send, f_recv,
    y_f_send, y_f_recv, y_t_send, y_t_recv, y_y_send, y_y_recv, y_p_send, y_p_recv, c_send, c_recv, own, x_own, y_own, v_own,
):
    n_row, n_col, n_in, slots, own_j, rank, width, cols = dims
    js = own_j * rank
    half = js // 2
    kr = slots * rank
    total = n_row * width
    share = total // n_in
    group = n_col // n_in
    planes = n_row // 2
    zrows = js // n_row
    row, col, inner = lax.axis_index("row"), lax.axis_index("col"), lax.axis_index("inner")
    plane = lax.div(row, 2)
    parity = lax.rem(row, 2)
    twin = {"row": row + 1 - 2 * parity}
    far_planes = [lax.rem(plane + f, planes) for f in range(1, planes)]
    back_planes = [lax.rem(plane + planes - f, planes) for f in range(1, planes)]
    fars = [{"row": 2 * p + parity} for p in far_planes]
    up, down = {"col": lax.rem(col + 1, n_col)}, {"col": lax.rem(col + n_col - 1, n_col)}
    has = (col < n_col - 1, col > 0)
    middle = jnp.logical_and(has[0], has[1])
    beside = (col + 1 < n_col - 1, col - 1 > 0)
    row_peers = [lax.rem(row + d, n_row) for d in range(1, n_row)]
    in_peers = [lax.rem(inner + e, n_in) for e in range(1, n_in)]
    home = lax.div(col, group)
    helper = lax.rem(home + 1, n_in)
    helped = lax.rem(inner + n_in - 1, n_in)
    mine = pl.ds(pl.multiple_of(parity * half, half), half)

    def at_rows(s):
        return pl.ds(pl.multiple_of(s * js, js), js)

    def x_at(s, k, p, q):
        return xg.at[k, at_rows(s), pl.ds(pl.multiple_of((2 * p + q) * width, width), width)]

    def v_at(s):
        return vg.at[:, :, pl.ds(pl.multiple_of(s * cols, cols), cols)]

    def z_at(s, p, q):
        return zt.at[s, pl.ds(pl.multiple_of((2 * p + q) * zrows, zrows), zrows)]

    def y_at(k, p, q):
        return yg.at[k, :, pl.ds(pl.multiple_of((2 * p + q) * width, width), width)]

    def x_line(s, k, way, src=None):
        place = x_at(s, k, plane, parity)
        return remote(
            place if src is None else src, place, x_z_send.at[way, s, k], x_z_recv.at[s, k], (up, down)[way]
        )

    def x_far(s, k, f, src=None):
        place = x_at(s, k, plane, parity)
        return remote(place if src is None else src, place, x_f_send.at[f, s, k], x_f_recv.at[f, s, k], fars[f])

    def x_twin(s, k, p, src=None):
        place = x_at(s, k, p, parity)
        return remote(place if src is None else src, place, x_t_send.at[p, s, k], x_t_recv.at[p, s, k], twin)

    def z_line(s, way, src=None):
        place = z_at(s, plane, parity)
        return remote(place if src is None else src, place, z_z_send.at[way, s], z_z_recv.at[s], (up, down)[way])

    def z_far(s, f, src=None):
        place = z_at(s, plane, parity)
        return remote(place if src is None else src, place, z_f_send.at[f, s], z_f_recv.at[f, s], fars[f])

    def z_twin(s, p, src=None):
        place = z_at(s, p, parity)
        return remote(place if src is None else src, place, z_t_send.at[p, s], z_t_recv.at[p, s], twin)

    def v_line(s, way, src=None):
        return remote(
            v_at(s) if src is None else src, v_at(s), v_send.at[way, s], v_recv.at[s], (up, down)[way]
        )

    def z_piece(d):
        rows = pl.ds(pl.multiple_of(row_peers[d] * zrows, zrows), zrows)
        return remote(zpart.at[rows], zgot.at[d], zp_send.at[d], zp_recv.at[d], {"row": row_peers[d]})

    def x_side(k, f, way):
        place = x_at(col, k, back_planes[f], parity)
        return remote(place, place, x_s_send.at[f, way, k], x_s_recv.at[f, way, k], (up, down)[way])

    def y_far(f, k):
        return remote(y_at(k, plane, parity), y_at(k, plane, parity), y_f_send.at[f, k], y_f_recv.at[f, k], fars[f])

    def y_twin(p, k, src=None):
        place = y_at(k, p, parity)
        return remote(place if src is None else src, place, y_t_send.at[p, k], y_t_recv.at[p, k], twin)

    def y_inner(e, k):
        lane = pl.ds(pl.multiple_of(in_peers[e] * share, share), share)
        return remote(
            yg.at[k, mine, lane], yb.at[e, k, mine], y_y_send.at[e, k], y_y_recv.at[e, k], {"inner": in_peers[e]}
        )

    def y_pass(e, k):
        return remote(yb.at[e, k, mine], yb.at[e, k, mine], y_p_send.at[e, k], y_p_recv.at[e, k], twin)

    def share_plane(peer):
        return lax.div(peer * share, 2 * width)

    def s_peer(s, j, e):
        rows = pl.ds(j * rank, rank)
        return remote(
            ssend.at[s, rows], sgot.at[e, s, rows], s_send.at[e, s, j], s_recv.at[e, s, j], {"inner": in_peers[e]}
        )

    def m_home(s, h, source):
        return remote(msend.at[s, h], mgot.at[source, h], m_send.at[s, h], m_recv.at[source, h], {"col": s})

    def home_at(g, h):
        return s_home.at[pl.ds(h * half, half), pl.ds(pl.multiple_of(g * cols, cols), cols)]

    def h_home(s, g):
        return remote(hsend.at[s, pl.ds(0, half)], home_at(g, 0), h_send.at[s], h_recv.at[g], {"col": s})

    def h_relay(s, g):
        return remote(hsend.at[s, pl.ds(half, half)], hrel.at[g], r_send.at[s], r_recv.at[g], {"col": s})

    def h_pass(g, src=None):
        return remote(
            hrel.at[g] if src is None else src, home_at(g, 1), f_send.at[g], f_recv.at[g], {"inner": helped}
        )

    def c_inner(e):
        return remote(cross_pass, cross_got.at[e], c_send.at[e], c_recv.at[e], {"inner": in_peers[e]})

    def unit(b):
        both = jnp.minimum(col, n_col - 1 - col)
        near = lax.div(b + 1, 2)
        paired = jnp.where(lax.rem(b, 2) == 1, col - near, col + near)
        single = jnp.where(col < n_col - 1 - col, col + (b - both), col - (b - both))
        return jnp.where(b <= 2 * both, paired, single)

    def own_line(k):
        for way in range(2):

            @pl.when(has[way])
            def _(way=way):
                x_line(col, k, way).start()

    here_rows = pl.ds(pl.multiple_of(row * width, width), width)
    x_in = [
        pltpu.make_async_copy(x_hbm.at[k], x_at(col, k, plane, parity), x_own.at[k]) for k in range(slots)
    ]
    v_in = pltpu.make_async_copy(v_hbm, v_at(col), v_own.at[0])
    y_in = [pltpu.make_async_copy(y_hbm.at[k], y_at(k, plane, parity), y_own.at[k]) for k in range(slots)]
    o_in = pltpu.make_async_copy(o_hbm.at[:, :, here_rows], o_ref, v_own.at[1])
    u_in = pltpu.make_async_copy(u_hbm, u_ref, v_own.at[2])
    for fetch in [v_in] + x_in + y_in + [o_in, u_in]:
        fetch.start()
    for k in range(slots):
        pltpu.make_async_copy(d_ref.at[k], deff.at[k], own.at[k]).start()

    for fetch in [v_in] + x_in:
        fetch.wait()
    for fetch in y_in + [o_in, u_in]:
        fetch.wait()
    for j in range(own_j):
        inner_rows = jnp.concatenate(
            [yg[k, j * rank : (j + 1) * rank, here_rows] for k in range(slots)], axis=0
        )
        part = lax.dot_general(o_ref[j], inner_rows, NT, preferred_element_type=WIDE)
        zpart[j * rank : (j + 1) * rank, 0:kr] = part
    meet(
        [{"row": r} for r in row_peers]
        + [{"col": lax.rem(col + d, n_col)} for d in range(1, n_col)]
        + [{"inner": p} for p in in_peers]
    )

    for way in range(2):

        @pl.when(has[way])
        def _(way=way):
            v_line(col, way).start()

    for k in range(min(2, slots)):
        own_line(k)
    for f in range(planes - 1):
        x_far(col, 0, f).start()
    for k in range(slots):
        y_twin(plane, k).start()
    for k in range(slots):
        x_twin(col, k, plane).start()

    for d in range(n_row - 1):
        z_piece(d).start()
    for k in range(1, slots):
        for f in range(planes - 1):
            x_far(col, k, f).start()
    for k in range(slots):
        y_twin(plane, k).wait_recv()
    for e in range(n_in - 1):

        @pl.when(share_plane(in_peers[e]) == plane)
        def _(e=e):
            for k in range(slots):
                y_inner(e, k).start()

    def gather_z():
        total_z = zpart[pl.ds(pl.multiple_of(row * zrows, zrows), zrows), 0:kr]
        for d in range(n_row - 1):
            z_piece(d).wait_recv()
            total_z = total_z + zgot[d, :, 0:kr]
        quarter = total_z.astype(NARROW)
        zown[:, 0:kr] = quarter
        zt[col, pl.ds(pl.multiple_of(row * zrows, zrows), zrows), 0:kr] = quarter
        for way in range(2):

            @pl.when(has[way])
            def _(way=way):
                z_line(col, way, zown).start()

        for f in range(planes - 1):
            z_far(col, f, zown).start()
        z_twin(col, plane, zown).start()

    def along(t, act):
        for way in range(2):
            s = col - t if way == 0 else col + t

            @pl.when(s >= 0 if way == 0 else s < n_col)
            def _(s=s, way=way):
                act(s, way)

    def pass_v(s, way):
        v_line(s, way).wait_recv()

        @pl.when(has[way])
        def _():
            v_line(s, way).start()

    def pass_z(s, way):
        z_line(s, way).wait_recv()

        @pl.when(has[way])
        def _():
            z_line(s, way).start()

        z_twin(s, plane).start()

    def pump(b, k):
        def pass_x(s, way):
            x_line(s, k, way).wait_recv()

            @pl.when(has[way])
            def _():
                x_line(s, k, way).start()

            x_twin(s, k, plane).start()

            @pl.when(jnp.logical_not(jnp.logical_and(middle, b == 0)))
            def _():
                for f in range(planes - 1):
                    x_far(s, k, f).start()

        along(b + 1, pass_x)
        here = unit(b)

        @pl.when(jnp.logical_and(k == 0, b > 0))
        def _():
            along(b, pass_z)
            for f in range(planes - 1):
                z_far(here, f).start()

        below = jnp.logical_and(middle, here == col - 1)
        above = jnp.logical_and(middle, here == col + 1)
        for f in range(planes - 1):

            @pl.when(below)
            def _(f=f):
                x_side(k, f, 0).wait_recv()

            @pl.when(above)
            def _(f=f):
                x_side(k, f, 1).wait_recv()

            @pl.when(jnp.logical_not(jnp.logical_or(below, above)))
            def _(f=f):
                x_far(here, k, f).wait_recv()

            for way in range(2):

                @pl.when(jnp.logical_and(b == 0, beside[way]))
                def _(f=f, way=way):
                    x_side(k, f, way).start()

            x_twin(here, k, back_planes[f]).start()

        @pl.when(k == slots - 1)
        def _():
            for f in range(planes - 1):
                z_far(here, f).wait_recv()
                z_twin(here, back_planes[f]).start()

    step_rows = min(512, total)

    def effective(k):
        pltpu.make_async_copy(d_ref.at[k], deff.at[k], own.at[k]).wait()
        near = jnp.full((1, cols), flag_ref[0, k], jnp.int32) > 0

        def some(i, carry):
            at = pl.ds(pl.multiple_of(i * step_rows, step_rows), step_rows)
            low = lax.dot_general(vg[k, :, at], u_ref[k], TN, preferred_element_type=WIDE)
            dense = deff[k, at, :].astype(WIDE)
            deff[k, at, :] = jnp.where(near, dense, low).astype(NARROW)
            return carry

        lax.fori_loop(0, total // step_rows, some, 0)

    def piece(b, k):
        @pl.when(b == 0)
        def _():
            effective(k)

        s = unit(b)
        for p in range(planes):
            x_twin(s, k, p).wait_recv()
        out = jnp.dot(xg[k, at_rows(s), :], deff[k], preferred_element_type=WIDE).astype(NARROW)
        for j in range(own_j):
            pbuf[s, j, pl.ds(pl.multiple_of(k * rank, rank), rank), :] = out[j * rank : (j + 1) * rank]

    def sample(b):
        s = unit(b)
        for p in range(planes):
            z_twin(s, p).wait_recv()
        for j in range(own_j):
            rows = slice(j * rank, (j + 1) * rank)
            part = jnp.dot(zt[s, rows, 0:kr], pbuf[s, j], preferred_element_type=WIDE)
            spart[s, rows, :] = part
            ssend[s, rows, :] = part.astype(NARROW)
            for e in range(n_in - 1):
                s_peer(s, j, e).start()

    def finish(b):
        s = unit(b)
        away = s != col
        lane = lax.rem(col, group)
        for h in range(2):
            lows = []
            for i in range(own_j // 2):
                j = h * (own_j // 2) + i
                rows = slice(j * rank, (j + 1) * rank)
                for e in range(n_in - 1):
                    s_peer(s, j, e).wait_recv()
                whole = spart[s, rows, :]
                for e in range(n_in - 1):
                    whole = whole + sgot[e, s, rows, :].astype(WIDE)
                high, low = split(whole)
                hsend[s, rows, :] = high
                left = jnp.concatenate([high, low], axis=0)
                right = jnp.concatenate([pbuf[s, j], left], axis=0)
                both = lax.dot_general(left, right, NT, preferred_element_type=WIDE)
                top, under = both[:rank], both[rank:]
                cross = top[:, :kr] + under[:, :kr]
                gram = top[:, kr : kr + rank] + top[:, kr + rank :] + under[:, kr : kr + rank]
                gram_high, gram_low = split(gram)
                at = slice(i * rank, (i + 1) * rank)
                msend[s, h, at, 0:kr] = cross.astype(NARROW)
                msend[s, h, at, kr : kr + rank] = gram_high
                lows.append(gram_low)
            pair = jnp.concatenate(lows, axis=1)
            folds = (kr + rank) // pair.shape[1]
            deep = rank // folds
            msend[s, h, half : half + deep] = jnp.concatenate(
                [pair[i * deep : (i + 1) * deep] for i in range(folds)], axis=1
            )

            @pl.when(away)
            def _(h=h):
                m_home(s, h, col).start()

            if h == 0:

                @pl.when(jnp.logical_and(away, home == inner))
                def _():
                    h_home(s, lane).start()

            else:

                @pl.when(jnp.logical_and(away, helper == inner))
                def _():
                    h_relay(s, lane).start()

        @pl.when(jnp.logical_not(away))
        def _():
            mgot[col] = msend[s]

            @pl.when(home == inner)
            def _():
                s_home[0:half, pl.ds(pl.multiple_of(lane * cols, cols), cols)] = hsend[s, 0:half]

    count = n_col * slots
    ready = n_col - 2

    def done(q):
        return jnp.maximum(jnp.minimum(q, 2 * (q - ready + 1)), 0)

    def work(i, carry):
        b, k = lax.div(i, slots), lax.rem(i, slots)
        piece(b, k)

        @pl.when(k == slots - 1)
        def _():
            sample(b)

        @pl.when(jnp.logical_and(k == min(1, slots - 1), b > 0))
        def _():
            finish(b - 1)

        return carry

    def start_y():
        for f in range(planes - 1):
            for k in range(slots):
                y_far(f, k).start()

    def pass_y():
        for k in range(slots):
            for f in range(planes - 1):
                y_far(f, k).wait_recv()
                y_twin(back_planes[f], k).start()
            for f in range(planes - 1):
                y_twin(back_planes[f], k).wait_recv()
            for e in range(n_in - 1):

                @pl.when(share_plane(in_peers[e]) != plane)
                def _(e=e, k=k):
                    y_inner(e, k).start()

    def step(q, carry):
        @pl.when(q < count)
        def _():
            pump(lax.div(q, slots), lax.rem(q, slots))

        @pl.when(q < n_col - 1)
        def _():
            along(q + 1, pass_v)

        @pl.when(q + 2 < slots)
        def _():
            own_line(q + 2)

        @pl.when(q == 0)
        def _():
            gather_z()

        @pl.when(q == jnp.where(middle, 0, (n_col - 1) * slots))
        def _():
            start_y()

        @pl.when(jnp.logical_and(middle, q == 2 * slots))
        def _():
            pass_y()

        lax.fori_loop(done(q - 1), done(q), work, 0)
        return carry

    lax.fori_loop(0, count + 1, step, 0)
    finish(n_col - 1)

    @pl.when(jnp.logical_not(middle))
    def _():
        pass_y()

    for g in range(group):
        source = helped * group + g

        @pl.when(source != col)
        def _(g=g, source=source):
            h_relay(source, g).wait_recv()
            h_pass(g).start()

        @pl.when(source == col)
        def _(g=g):
            h_pass(g, hsend.at[col, pl.ds(half, half)]).start()

    for d in range(1, n_col):
        source = lax.rem(col + d, n_col)
        for h in range(2):
            m_home(source, h, source).wait_recv()
    grams = []
    for h in range(2):
        crosses = mgot[0, h, 0:half, 0:kr].astype(WIDE)
        high = mgot[0, h, 0:half, kr : kr + rank].astype(WIDE)
        deep = msend.shape[2] - half
        under = mgot[0, h, half : half + deep].astype(WIDE)
        for c in range(1, n_col):
            crosses = crosses + mgot[c, h, 0:half, 0:kr].astype(WIDE)
            high = high + mgot[c, h, 0:half, kr : kr + rank].astype(WIDE)
            under = under + mgot[c, h, half : half + deep].astype(WIDE)
        cross_sum[h * half : (h + 1) * half, 0:kr] = crosses
        cross_pass[h * half : (h + 1) * half, 0:kr] = crosses.astype(NARROW)
        wide = half
        pair = jnp.concatenate([under[:, i * wide : (i + 1) * wide] for i in range(under.shape[1] // wide)], axis=0)
        for i in range(own_j // 2):
            grams.append(high[i * rank : (i + 1) * rank] + pair[:, i * rank : (i + 1) * rank])
    for e in range(n_in - 1):
        c_inner(e).start()
    inverse_factor(grams, inv)

    for g in range(group):
        source = inner * group + g

        @pl.when(source != col)
        def _(g=g, source=source):
            h_home(source, g).wait_recv()

        h_pass(g).wait_recv()
    for e in range(n_in - 1):
        for k in range(slots):
            y_inner(e, k).wait_recv()
            y_pass(e, k).start()
    for j in range(own_j):
        rows = slice(j * rank, (j + 1) * rank)
        both = jnp.concatenate(split(inv[j]), axis=0)
        out = jnp.dot(both, s_home[rows, :], preferred_element_type=WIDE)
        basis_ref[j] = out[:rank] + out[rank:]
    for e in range(n_in - 1):
        c_inner(e).wait_recv()
    left = []
    for j in range(own_j):
        rows = slice(j * rank, (j + 1) * rank)
        crossed = jnp.concatenate(
            [cross_sum[rows, 0:kr]] + [cross_got[e, rows, 0:kr].astype(WIDE) for e in range(n_in - 1)], axis=1
        )
        projected = jnp.dot(inv[j], crossed, precision=HIGHEST, preferred_element_type=WIDE)
        left.append(jnp.concatenate(split(projected), axis=0))
    for e in range(n_in - 1):
        for k in range(slots):
            y_pass(e, k).wait_recv()
    lane_own = pl.ds(pl.multiple_of(inner * share, share), share)
    for j in range(own_j):
        rows = slice(j * rank, (j + 1) * rank)
        right = [yg[k, rows, lane_own] for k in range(slots)]
        right += [yb[e, k, rows, :] for e in range(n_in - 1) for k in range(slots)]
        out = jnp.dot(left[j], jnp.concatenate(right, axis=0), preferred_element_type=WIDE)
        coupling_ref[j] = out[:rank] + out[rank:]

    for k in range(slots):
        for p in range(planes):
            y_twin(p, k).wait_send()
        for f in range(planes - 1):
            y_far(f, k).wait_send()
            for way in range(2):

                @pl.when(beside[way])
                def _(f=f, k=k, way=way):
                    x_side(k, f, way).wait_send()

    for d in range(n_row - 1):
        z_piece(d).wait_send()
    for e in range(n_in - 1):
        for k in range(slots):
            y_inner(e, k).wait_send()
            y_pass(e, k).wait_send()
        c_inner(e).wait_send()
    for g in range(group):
        h_pass(g).wait_send()

    def drain(s, carry):
        for way in range(2):

            @pl.when(jnp.logical_and(has[way], s <= col if way == 0 else s >= col))
            def _(way=way):
                v_line(s, way).wait_send()
                z_line(s, way).wait_send()
                for k in range(slots):
                    x_line(s, k, way).wait_send()

        for f in range(planes - 1):
            z_far(s, f).wait_send()

            @pl.when(jnp.logical_not(jnp.logical_and(middle, jnp.logical_or(s == col - 1, s == col + 1))))
            def _(f=f):
                for k in range(slots):
                    x_far(s, k, f).wait_send()

        for p in range(planes):
            z_twin(s, p).wait_send()
            for k in range(slots):
                x_twin(s, k, p).wait_send()
        for e in range(n_in - 1):
            for j in range(own_j):
                s_peer(s, j, e).wait_send()

        @pl.when(s != col)
        def _():
            for h in range(2):
                m_home(s, h, col).wait_send()

            @pl.when(home == inner)
            def _():
                h_home(s, 0).wait_send()

            @pl.when(helper == inner)
            def _():
                h_relay(s, 0).wait_send()

        return carry

    lax.fori_loop(0, n_col, drain, 0)


def product(flags, u, v, d, x, y, omega, sizes):
    n_row, n_col, n_in = sizes
    slots, js, width = x.shape
    own_j, rank, total = omega.shape
    cols = u.shape[-1]
    planes = n_row // 2
    kr = slots * rank
    group = n_col // n_in
    share = total // n_in
    half = js // 2
    packed = half + rank * (own_j // 2) * rank // (kr + rank)
    vmem = pl.BlockSpec(memory_space=pltpu.VMEM)
    dma = pltpu.SemaphoreType.DMA
    dims = (n_row, n_col, n_in, slots, own_j, rank, width, cols)
    out = jax.ShapeDtypeStruct((own_j, rank, share), WIDE)
    buffers = [
        (u.shape, NARROW),
        ((own_j, rank, width), NARROW),
        ((slots, n_col * js, total), NARROW),
        ((slots, rank, total), NARROW),
        ((slots, js, total), NARROW),
        ((n_in - 1, slots, js, share), NARROW),
        ((slots, total, cols), NARROW),
        ((n_col, own_j, kr, cols), NARROW),
        ((n_col, js, lanes(kr)), NARROW),
        ((js, lanes(kr)), WIDE),
        ((n_row - 1, js // n_row, lanes(kr)), WIDE),
        ((js // n_row, lanes(kr)), NARROW),
        ((n_col, js, cols), WIDE),
        ((n_col, js, cols), NARROW),
        ((n_in - 1, n_col, js, cols), NARROW),
        ((n_col, 2, packed, kr + rank), NARROW),
        ((n_col, 2, packed, kr + rank), NARROW),
        ((n_col, js, cols), NARROW),
        ((group, half, cols), NARROW),
        ((js, share), NARROW),
        ((js, lanes(kr)), WIDE),
        ((js, lanes(kr)), NARROW),
        ((n_in - 1, js, lanes(kr)), NARROW),
        ((own_j, rank, rank), WIDE),
    ]
    held = sum(math.prod(shape) * jnp.dtype(kind).itemsize for shape, kind in buffers)
    return pl.pallas_call(
        functools.partial(product_kernel, dims),
        out_shape=(out, out),
        in_specs=[pl.BlockSpec(memory_space=pltpu.SMEM)] + [pl.BlockSpec(memory_space=pltpu.HBM)] * 6,
        out_specs=[vmem] * 2,
        scratch_shapes=[pltpu.VMEM(*buffer) for buffer in buffers] + [
            dma((2, n_col, slots)), dma((n_col, slots)),
            dma((planes - 1, n_col, slots)), dma((planes - 1, n_col, slots)),
            dma((planes, n_col, slots)), dma((planes, n_col, slots)),
            dma((planes - 1, 2, slots)), dma((planes - 1, 2, slots)),
            dma((2, n_col)), dma((n_col,)),
            dma((2, n_col)), dma((n_col,)),
            dma((planes - 1, n_col)), dma((planes - 1, n_col)),
            dma((planes, n_col)), dma((planes, n_col)),
            dma((n_row - 1,)), dma((n_row - 1,)),
            dma((n_in - 1, n_col, own_j)), dma((n_in - 1, n_col, own_j)),
            dma((n_col, 2)), dma((n_col, 2)),
            dma((n_col,)), dma((group,)),
            dma((n_col,)), dma((group,)),
            dma((group,)), dma((group,)),
            dma((planes - 1, slots)), dma((planes - 1, slots)),
            dma((planes, slots)), dma((planes, slots)),
            dma((n_in - 1, slots)), dma((n_in - 1, slots)),
            dma((n_in - 1, slots)), dma((n_in - 1, slots)),
            dma((n_in - 1,)), dma((n_in - 1,)),
            dma((slots,)), dma((slots,)), dma((slots,)), dma((3,)),
        ],
        compiler_params=pltpu.CompilerParams(
            collective_id=0, has_side_effects=True, vmem_limit_bytes=held + 6 * 1024 * 1024
        ),
    )(flags, *[pltpu.with_memory_space_constraint(part, pltpu.HBM) for part in (u, v, d, x, y, omega)])


def inverse_factor(gram, out_ref):
    count, size = len(gram), gram[0].shape[0]
    tall = lax.broadcasted_iota(jnp.int32, (size, size), 0)
    wide = lax.broadcasted_iota(jnp.int32, (size, size), 1)
    eye = (tall == wide).astype(WIDE)
    lines = lax.broadcasted_iota(jnp.int32, (8, 1), 0)
    works = []
    for j in range(count):
        full = jnp.concatenate([gram[j], eye], axis=1)
        works.append([full[8 * b : 8 * b + 8] for b in range(size // 8)])
    scales = [[] for _ in range(count)]
    for k in range(size):
        b0, in_b = k // 8, k % 8
        for j in range(count):
            work = works[j]
            line = work[b0][in_b : in_b + 1]
            pivot = line[:, k : k + 1]
            scales[j].append(lax.rsqrt(pivot))
            line = line * (1.0 / pivot)
            for b in range(b0, size // 8):
                column = work[b][:, k : k + 1]
                if b == b0:
                    if in_b == 7:
                        continue
                    column = jnp.where(lines > in_b, column, 0.0)
                work[b] = work[b] - column * line
    for j in range(count):
        scale = jnp.concatenate(scales[j], axis=0)
        out_ref[j] = jnp.concatenate(works[j], axis=0)[:, size:] * scale


def local(sizes, near_flags, row_factor, col_factor, near_block, inner_left, inner_right, sketch_matrix):
    slots, own_j, rank, width = inner_left.shape
    js = own_j * rank
    basis, coupling = product(
        near_flags, row_factor[0], col_factor[0], near_block[0],
        inner_left.reshape(slots, js, width), inner_right.reshape(slots, js, width), sketch_matrix, sizes,
    )
    return (basis[None] * math.sqrt(width * sizes[0]), coupling[None])


def solution(mesh):
    sizes = (mesh.shape["row"], mesh.shape["col"], mesh.shape["inner"])
    in_specs = (
        P("row", "inner"),
        P("row", "inner", None, "col"),
        P("row", "inner", None, "col"),
        P("row", "inner", None, "col"),
        P("inner", "col", None, "row"),
        P("inner", "col", None, "row"),
        P("col", None, None),
    )
    out_specs = (P("row", "col", None, "inner"), P("row", "col", None, "inner"))
    return jax.shard_map(
        functools.partial(local, sizes), mesh=mesh, in_specs=in_specs, out_specs=out_specs, check_vma=False
    )
```

```python
import functools
import math

import jax
import jax.numpy as jnp
from jax import lax
from jax.experimental import pallas as pl
from jax.experimental.pallas import tpu as pltpu
from jax.sharding import PartitionSpec as P

MESH = pl.DeviceIdType.MESH
HIGHEST = lax.Precision.HIGHEST
WIDE = jnp.float32
NARROW = jnp.bfloat16
NT = (((1,), (1,)), ((), ()))
TN = (((0,), (0,)), ((), ()))


def remote(src, dst, send, recv, device):
    return pltpu.make_async_remote_copy(
        src_ref=src, dst_ref=dst, send_sem=send, recv_sem=recv, device_id=device, device_id_type=MESH
    )


def meet(devices):
    barrier = pltpu.get_barrier_semaphore()
    for device in devices:
        pl.semaphore_signal(barrier, inc=1, device_id=device, device_id_type=MESH)
    pl.semaphore_wait(barrier, len(devices))


def split(value):
    high = value.astype(NARROW)
    return high, (value - high.astype(WIDE)).astype(NARROW)


def lanes(length):
    return -(-length // 128) * 128


def product_kernel(
    dims, flag_ref, u_hbm, v_hbm, d_ref, x_hbm, y_hbm, o_hbm,
    basis_ref, coupling_ref,
    u_ref, o_ref,
    xg, vg, yg, yb, deff, pbuf, zt, zpart, zgot, zown, spart, ssend, sgot, msend, mgot, hsend, hrel, s_home,
    cross_sum, cross_pass, cross_got, inv,
    x_z_send, x_z_recv, x_f_send, x_f_recv, x_t_send, x_t_recv, x_s_send, x_s_recv,
    v_send, v_recv, z_z_send, z_z_recv, z_f_send, z_f_recv, z_t_send, z_t_recv, zp_send, zp_recv,
    s_send, s_recv, m_send, m_recv, h_send, h_recv, r_send, r_recv, f_send, f_recv,
    y_f_send, y_f_recv, y_t_send, y_t_recv, y_y_send, y_y_recv, y_p_send, y_p_recv, c_send, c_recv,
    w_send, w_recv, own, x_own, y_own, v_own,
):
    n_row, n_col, n_in, slots, own_j, rank, width, cols = dims
    js = own_j * rank
    half = js // 2
    kr = slots * rank
    total = n_row * width
    share = total // n_in
    group = n_col // n_in
    planes = n_row // 2
    zrows = js // n_row
    row, col, inner = lax.axis_index("row"), lax.axis_index("col"), lax.axis_index("inner")
    plane = lax.div(row, 2)
    parity = lax.rem(row, 2)
    twin = {"row": row + 1 - 2 * parity}
    far_planes = [lax.rem(plane + f, planes) for f in range(1, planes)]
    back_planes = [lax.rem(plane + planes - f, planes) for f in range(1, planes)]
    fars = [{"row": 2 * p + parity} for p in far_planes]
    up, down = {"col": lax.rem(col + 1, n_col)}, {"col": lax.rem(col + n_col - 1, n_col)}
    has = (col < n_col - 1, col > 0)
    middle = jnp.logical_and(has[0], has[1])
    beside = (col + 1 < n_col - 1, col - 1 > 0)
    row_peers = [lax.rem(row + d, n_row) for d in range(1, n_row)]
    in_peers = [lax.rem(inner + e, n_in) for e in range(1, n_in)]
    home = lax.div(col, group)
    helper = lax.rem(home + 1, n_in)
    helped = lax.rem(inner + n_in - 1, n_in)
    mine = pl.ds(pl.multiple_of(parity * half, half), half)

    def at_rows(s):
        return pl.ds(pl.multiple_of(s * js, js), js)

    def x_at(s, k, p, q):
        return xg.at[k, at_rows(s), pl.ds(pl.multiple_of((2 * p + q) * width, width), width)]

    def v_at(s):
        return vg.at[:, :, pl.ds(pl.multiple_of(s * cols, cols), cols)]

    def z_at(s, p, q):
        return zt.at[s, pl.ds(pl.multiple_of((2 * p + q) * zrows, zrows), zrows)]

    def y_at(k, p, q):
        return yg.at[k, :, pl.ds(pl.multiple_of((2 * p + q) * width, width), width)]

    def x_line(s, k, way, src=None):
        place = x_at(s, k, plane, parity)
        return remote(
            place if src is None else src, place, x_z_send.at[way, s, k], x_z_recv.at[s, k], (up, down)[way]
        )

    def x_far(s, k, f, src=None):
        place = x_at(s, k, plane, parity)
        return remote(place if src is None else src, place, x_f_send.at[f, s, k], x_f_recv.at[f, s, k], fars[f])

    def x_twin(s, k, p, src=None):
        place = x_at(s, k, p, parity)
        return remote(place if src is None else src, place, x_t_send.at[p, s, k], x_t_recv.at[p, s, k], twin)

    def z_line(s, way, src=None):
        place = z_at(s, plane, parity)
        return remote(place if src is None else src, place, z_z_send.at[way, s], z_z_recv.at[s], (up, down)[way])

    def z_far(s, f, src=None):
        place = z_at(s, plane, parity)
        return remote(place if src is None else src, place, z_f_send.at[f, s], z_f_recv.at[f, s], fars[f])

    def z_twin(s, p, src=None):
        place = z_at(s, p, parity)
        return remote(place if src is None else src, place, z_t_send.at[p, s], z_t_recv.at[p, s], twin)

    def v_line(s, way, src=None):
        return remote(
            v_at(s) if src is None else src, v_at(s), v_send.at[way, s], v_recv.at[s], (up, down)[way]
        )

    def z_piece(d):
        rows = pl.ds(pl.multiple_of(row_peers[d] * zrows, zrows), zrows)
        return remote(zpart.at[rows], zgot.at[d], zp_send.at[d], zp_recv.at[d], {"row": row_peers[d]})

    def x_side(k, f, way):
        place = x_at(col, k, back_planes[f], parity)
        return remote(place, place, x_s_send.at[f, way, k], x_s_recv.at[f, way, k], (up, down)[way])

    def y_far(f, k):
        return remote(y_at(k, plane, parity), y_at(k, plane, parity), y_f_send.at[f, k], y_f_recv.at[f, k], fars[f])

    def y_twin(p, k, src=None):
        place = y_at(k, p, parity)
        return remote(place if src is None else src, place, y_t_send.at[p, k], y_t_recv.at[p, k], twin)

    def y_inner(e, k):
        lane = pl.ds(pl.multiple_of(in_peers[e] * share, share), share)
        return remote(
            yg.at[k, mine, lane], yb.at[e, k, mine], y_y_send.at[e, k], y_y_recv.at[e, k], {"inner": in_peers[e]}
        )

    def y_pass(e, k):
        return remote(yb.at[e, k, mine], yb.at[e, k, mine], y_p_send.at[e, k], y_p_recv.at[e, k], twin)

    def share_plane(peer):
        return lax.div(peer * share, 2 * width)

    def y_cross(f, e):
        place = yb.at[e, slots - 1, mine]
        return remote(place, place, w_send.at[f, e], w_recv.at[f, e], fars[f])

    own_share = share_plane(inner) == plane

    def crosses_back(f, k):
        return True if k < slots - 1 else share_plane(inner) == back_planes[f]

    def s_peer(s, j, e):
        rows = pl.ds(j * rank, rank)
        return remote(
            ssend.at[s, rows], sgot.at[e, s, rows], s_send.at[e, s, j], s_recv.at[e, s, j], {"inner": in_peers[e]}
        )

    def m_home(s, h, source):
        return remote(msend.at[s, h], mgot.at[source, h], m_send.at[s, h], m_recv.at[source, h], {"col": s})

    def home_at(g, h):
        return s_home.at[pl.ds(h * half, half), pl.ds(pl.multiple_of(g * cols, cols), cols)]

    def h_home(s, g):
        return remote(hsend.at[s, pl.ds(0, half)], home_at(g, 0), h_send.at[s], h_recv.at[g], {"col": s})

    def h_relay(s, g):
        return remote(hsend.at[s, pl.ds(half, half)], hrel.at[g], r_send.at[s], r_recv.at[g], {"col": s})

    def h_pass(g, src=None):
        return remote(
            hrel.at[g] if src is None else src, home_at(g, 1), f_send.at[g], f_recv.at[g], {"inner": helped}
        )

    def c_inner(e):
        return remote(cross_pass, cross_got.at[e], c_send.at[e], c_recv.at[e], {"inner": in_peers[e]})

    def unit(b):
        both = jnp.minimum(col, n_col - 1 - col)
        near = lax.div(b + 1, 2)
        paired = jnp.where(lax.rem(b, 2) == 1, col - near, col + near)
        single = jnp.where(col < n_col - 1 - col, col + (b - both), col - (b - both))
        return jnp.where(b <= 2 * both, paired, single)

    def own_line(k):
        for way in range(2):

            @pl.when(has[way])
            def _(way=way):
                x_line(col, k, way).start()

    here_rows = pl.ds(pl.multiple_of(row * width, width), width)
    x_in = [
        pltpu.make_async_copy(x_hbm.at[k], x_at(col, k, plane, parity), x_own.at[k]) for k in range(slots)
    ]
    v_in = pltpu.make_async_copy(v_hbm, v_at(col), v_own.at[0])
    y_in = [pltpu.make_async_copy(y_hbm.at[k], y_at(k, plane, parity), y_own.at[k]) for k in range(slots)]
    o_in = pltpu.make_async_copy(o_hbm.at[:, :, here_rows], o_ref, v_own.at[1])
    u_in = pltpu.make_async_copy(u_hbm, u_ref, v_own.at[2])
    for fetch in [v_in] + x_in + y_in + [o_in, u_in]:
        fetch.start()
    for k in range(slots):
        pltpu.make_async_copy(d_ref.at[k], deff.at[k], own.at[k]).start()

    for fetch in [v_in] + x_in:
        fetch.wait()
    for fetch in y_in + [o_in, u_in]:
        fetch.wait()
    for j in range(own_j):
        inner_rows = jnp.concatenate(
            [yg[k, j * rank : (j + 1) * rank, here_rows] for k in range(slots)], axis=0
        )
        part = lax.dot_general(o_ref[j], inner_rows, NT, preferred_element_type=WIDE)
        zpart[j * rank : (j + 1) * rank, 0:kr] = part
    meet(
        [{"row": r} for r in row_peers]
        + [{"col": lax.rem(col + d, n_col)} for d in range(1, n_col)]
        + [{"inner": p} for p in in_peers]
    )

    for way in range(2):

        @pl.when(has[way])
        def _(way=way):
            v_line(col, way).start()

    own_line(0)
    for f in range(planes - 1):
        x_far(col, 0, f).start()
    for k in range(slots):
        y_twin(plane, k).start()
    for k in range(slots):
        x_twin(col, k, plane).start()

    for d in range(n_row - 1):
        z_piece(d).start()
    for k in range(1, slots):
        for f in range(planes - 1):
            x_far(col, k, f).start()
    for k in range(slots):
        y_twin(plane, k).wait_recv()
    for e in range(n_in - 1):

        @pl.when(share_plane(in_peers[e]) == plane)
        def _(e=e):
            for k in range(slots):
                y_inner(e, k).start()

    def gather_z():
        total_z = zpart[pl.ds(pl.multiple_of(row * zrows, zrows), zrows), 0:kr]
        for d in range(n_row - 1):
            z_piece(d).wait_recv()
            total_z = total_z + zgot[d, :, 0:kr]
        quarter = total_z.astype(NARROW)
        zown[:, 0:kr] = quarter
        zt[col, pl.ds(pl.multiple_of(row * zrows, zrows), zrows), 0:kr] = quarter
        for way in range(2):

            @pl.when(has[way])
            def _(way=way):
                z_line(col, way, zown).start()

        for f in range(planes - 1):
            z_far(col, f, zown).start()
        z_twin(col, plane, zown).start()

    def along(t, act):
        for way in range(2):
            s = col - t if way == 0 else col + t

            @pl.when(s >= 0 if way == 0 else s < n_col)
            def _(s=s, way=way):
                act(s, way)

    def pass_v(s, way):
        v_line(s, way).wait_recv()

        @pl.when(has[way])
        def _():
            v_line(s, way).start()

    def pass_z(s, way):
        z_line(s, way).wait_recv()

        @pl.when(has[way])
        def _():
            z_line(s, way).start()

        z_twin(s, plane).start()

    def pump(b, k):
        def pass_x(s, way):
            x_line(s, k, way).wait_recv()

            @pl.when(has[way])
            def _():
                x_line(s, k, way).start()

            x_twin(s, k, plane).start()

            @pl.when(jnp.logical_not(jnp.logical_and(middle, b == 0)))
            def _():
                for f in range(planes - 1):
                    x_far(s, k, f).start()

        along(b + 1, pass_x)
        here = unit(b)

        @pl.when(jnp.logical_and(k == 0, b > 0))
        def _():
            along(b, pass_z)
            for f in range(planes - 1):
                z_far(here, f).start()

        below = jnp.logical_and(middle, here == col - 1)
        above = jnp.logical_and(middle, here == col + 1)
        for f in range(planes - 1):

            @pl.when(below)
            def _(f=f):
                x_side(k, f, 0).wait_recv()

            @pl.when(above)
            def _(f=f):
                x_side(k, f, 1).wait_recv()

            @pl.when(jnp.logical_not(jnp.logical_or(below, above)))
            def _(f=f):
                x_far(here, k, f).wait_recv()

            for way in range(2):

                @pl.when(jnp.logical_and(b == 0, beside[way]))
                def _(f=f, way=way):
                    x_side(k, f, way).start()

            x_twin(here, k, back_planes[f]).start()

        @pl.when(k == slots - 1)
        def _():
            for f in range(planes - 1):
                z_far(here, f).wait_recv()
                z_twin(here, back_planes[f]).start()

    step_rows = min(512, total)

    def effective(k):
        pltpu.make_async_copy(d_ref.at[k], deff.at[k], own.at[k]).wait()
        near = jnp.full((1, cols), flag_ref[0, k], jnp.int32) > 0

        def some(i, carry):
            at = pl.ds(pl.multiple_of(i * step_rows, step_rows), step_rows)
            low = lax.dot_general(vg[k, :, at], u_ref[k], TN, preferred_element_type=WIDE)
            dense = deff[k, at, :].astype(WIDE)
            deff[k, at, :] = jnp.where(near, dense, low).astype(NARROW)
            return carry

        lax.fori_loop(0, total // step_rows, some, 0)

    def piece(b, k):
        @pl.when(b == 0)
        def _():
            effective(k)

        s = unit(b)
        for p in range(planes):
            x_twin(s, k, p).wait_recv()
        out = jnp.dot(xg[k, at_rows(s), :], deff[k], preferred_element_type=WIDE).astype(NARROW)
        for j in range(own_j):
            pbuf[s, j, pl.ds(pl.multiple_of(k * rank, rank), rank), :] = out[j * rank : (j + 1) * rank]

    def sample(b):
        s = unit(b)
        for p in range(planes):
            z_twin(s, p).wait_recv()
        for j in range(own_j):
            rows = slice(j * rank, (j + 1) * rank)
            part = jnp.dot(zt[s, rows, 0:kr], pbuf[s, j], preferred_element_type=WIDE)
            spart[s, rows, :] = part
            ssend[s, rows, :] = part.astype(NARROW)
            for e in range(n_in - 1):
                s_peer(s, j, e).start()

    def finish(b):
        s = unit(b)
        away = s != col
        lane = lax.rem(col, group)
        for h in range(2):
            lows = []
            for i in range(own_j // 2):
                j = h * (own_j // 2) + i
                rows = slice(j * rank, (j + 1) * rank)
                for e in range(n_in - 1):
                    s_peer(s, j, e).wait_recv()
                whole = spart[s, rows, :]
                for e in range(n_in - 1):
                    whole = whole + sgot[e, s, rows, :].astype(WIDE)
                high, low = split(whole)
                hsend[s, rows, :] = high
                left = jnp.concatenate([high, low], axis=0)
                right = jnp.concatenate([pbuf[s, j], left], axis=0)
                both = lax.dot_general(left, right, NT, preferred_element_type=WIDE)
                top, under = both[:rank], both[rank:]
                cross = top[:, :kr] + under[:, :kr]
                gram = top[:, kr : kr + rank] + top[:, kr + rank :] + under[:, kr : kr + rank]
                gram_high, gram_low = split(gram)
                at = slice(i * rank, (i + 1) * rank)
                msend[s, h, at, 0:kr] = cross.astype(NARROW)
                msend[s, h, at, kr : kr + rank] = gram_high
                lows.append(gram_low)
            pair = jnp.concatenate(lows, axis=1)
            folds = (kr + rank) // pair.shape[1]
            deep = rank // folds
            msend[s, h, half : half + deep] = jnp.concatenate(
                [pair[i * deep : (i + 1) * deep] for i in range(folds)], axis=1
            )

            @pl.when(away)
            def _(h=h):
                m_home(s, h, col).start()

            if h == 0:

                @pl.when(jnp.logical_and(away, home == inner))
                def _():
                    h_home(s, lane).start()

            else:

                @pl.when(jnp.logical_and(away, helper == inner))
                def _():
                    h_relay(s, lane).start()

        @pl.when(jnp.logical_not(away))
        def _():
            mgot[col] = msend[s]

            @pl.when(home == inner)
            def _():
                s_home[0:half, pl.ds(pl.multiple_of(lane * cols, cols), cols)] = hsend[s, 0:half]

    count = n_col * slots
    ready = n_col - 2

    def done(q):
        return jnp.maximum(jnp.minimum(q, 2 * (q - ready + 1)), 0)

    def work(i, carry):
        b, k = lax.div(i, slots), lax.rem(i, slots)
        piece(b, k)

        @pl.when(k == slots - 1)
        def _():
            sample(b)

        @pl.when(jnp.logical_and(k == min(1, slots - 1), b > 0))
        def _():
            finish(b - 1)

        return carry

    def start_y():
        for f in range(planes - 1):
            for k in range(slots):

                @pl.when(own_share if k == slots - 1 else True)
                def _(f=f, k=k):
                    y_far(f, k).start()

    def cross_y():
        @pl.when(own_share)
        def _():
            for e in range(n_in - 1):
                y_inner(e, slots - 1).wait_recv()
                for f in range(planes - 1):
                    y_cross(f, e).start()

    def pass_y():
        for k in range(slots):
            for f in range(planes - 1):

                @pl.when(crosses_back(f, k))
                def _(f=f, k=k):
                    y_far(f, k).wait_recv()
                    y_twin(back_planes[f], k).start()

            for f in range(planes - 1):

                @pl.when(crosses_back(f, k))
                def _(f=f, k=k):
                    y_twin(back_planes[f], k).wait_recv()

            if k < slots - 1:
                for e in range(n_in - 1):

                    @pl.when(share_plane(in_peers[e]) != plane)
                    def _(e=e, k=k):
                        y_inner(e, k).start()

    def step(q, carry):
        @pl.when(q < n_col - 1)
        def _():
            along(q + 1, pass_v)

        @pl.when(q + 1 < slots)
        def _():
            own_line(q + 1)

        @pl.when(q < count)
        def _():
            pump(lax.div(q, slots), lax.rem(q, slots))


        @pl.when(q == 0)
        def _():
            gather_z()

        @pl.when(q == jnp.where(middle, 0, (n_col - 1) * slots))
        def _():
            start_y()

        @pl.when(q == jnp.where(middle, 2 * slots, (n_col - 1) * slots))
        def _():
            cross_y()

        @pl.when(jnp.logical_and(middle, q == 2 * slots))
        def _():
            pass_y()

        lax.fori_loop(done(q - 1), done(q), work, 0)
        return carry

    lax.fori_loop(0, count + 1, step, 0)
    finish(n_col - 1)

    @pl.when(jnp.logical_not(middle))
    def _():
        pass_y()

    for g in range(group):
        source = helped * group + g

        @pl.when(source != col)
        def _(g=g, source=source):
            h_relay(source, g).wait_recv()
            h_pass(g).start()

        @pl.when(source == col)
        def _(g=g):
            h_pass(g, hsend.at[col, pl.ds(half, half)]).start()

    for d in range(1, n_col):
        source = lax.rem(col + d, n_col)
        for h in range(2):
            m_home(source, h, source).wait_recv()
    grams = []
    for h in range(2):
        crosses = mgot[0, h, 0:half, 0:kr].astype(WIDE)
        high = mgot[0, h, 0:half, kr : kr + rank].astype(WIDE)
        deep = msend.shape[2] - half
        under = mgot[0, h, half : half + deep].astype(WIDE)
        for c in range(1, n_col):
            crosses = crosses + mgot[c, h, 0:half, 0:kr].astype(WIDE)
            high = high + mgot[c, h, 0:half, kr : kr + rank].astype(WIDE)
            under = under + mgot[c, h, half : half + deep].astype(WIDE)
        cross_sum[h * half : (h + 1) * half, 0:kr] = crosses
        cross_pass[h * half : (h + 1) * half, 0:kr] = crosses.astype(NARROW)
        wide = half
        pair = jnp.concatenate([under[:, i * wide : (i + 1) * wide] for i in range(under.shape[1] // wide)], axis=0)
        for i in range(own_j // 2):
            grams.append(high[i * rank : (i + 1) * rank] + pair[:, i * rank : (i + 1) * rank])
    for e in range(n_in - 1):
        c_inner(e).start()
    inverse_factor(grams, inv)

    for g in range(group):
        source = inner * group + g

        @pl.when(source != col)
        def _(g=g, source=source):
            h_home(source, g).wait_recv()

        h_pass(g).wait_recv()
    for e in range(n_in - 1):
        for k in range(slots - 1):
            y_inner(e, k).wait_recv()
            y_pass(e, k).start()
        for f in range(planes - 1):

            @pl.when(share_plane(inner) == back_planes[f])
            def _(e=e, f=f):
                y_cross(f, e).wait_recv()

        y_pass(e, slots - 1).start()
    for j in range(own_j):
        rows = slice(j * rank, (j + 1) * rank)
        both = jnp.concatenate(split(inv[j]), axis=0)
        out = jnp.dot(both, s_home[rows, :], preferred_element_type=WIDE)
        basis_ref[j] = out[:rank] + out[rank:]
    for e in range(n_in - 1):
        c_inner(e).wait_recv()
    left = []
    for j in range(own_j):
        rows = slice(j * rank, (j + 1) * rank)
        crossed = jnp.concatenate(
            [cross_sum[rows, 0:kr]] + [cross_got[e, rows, 0:kr].astype(WIDE) for e in range(n_in - 1)], axis=1
        )
        projected = jnp.dot(inv[j], crossed, precision=HIGHEST, preferred_element_type=WIDE)
        left.append(jnp.concatenate(split(projected), axis=0))
    for e in range(n_in - 1):
        for k in range(slots):
            y_pass(e, k).wait_recv()
    lane_own = pl.ds(pl.multiple_of(inner * share, share), share)
    for j in range(own_j):
        rows = slice(j * rank, (j + 1) * rank)
        right = [yg[k, rows, lane_own] for k in range(slots)]
        right += [yb[e, k, rows, :] for e in range(n_in - 1) for k in range(slots)]
        out = jnp.dot(left[j], jnp.concatenate(right, axis=0), preferred_element_type=WIDE)
        coupling_ref[j] = out[:rank] + out[rank:]

    for k in range(slots):
        y_twin(plane, k).wait_send()
        for f in range(planes - 1):

            @pl.when(crosses_back(f, k))
            def _(f=f, k=k):
                y_twin(back_planes[f], k).wait_send()

            @pl.when(own_share if k == slots - 1 else True)
            def _(f=f, k=k):
                y_far(f, k).wait_send()

            for way in range(2):

                @pl.when(beside[way])
                def _(f=f, k=k, way=way):
                    x_side(k, f, way).wait_send()

    for d in range(n_row - 1):
        z_piece(d).wait_send()
    for e in range(n_in - 1):
        for k in range(slots):
            y_pass(e, k).wait_send()

            @pl.when(share_plane(in_peers[e]) == plane if k == slots - 1 else True)
            def _(e=e, k=k):
                y_inner(e, k).wait_send()

        for f in range(planes - 1):

            @pl.when(own_share)
            def _(e=e, f=f):
                y_cross(f, e).wait_send()

        c_inner(e).wait_send()
    for g in range(group):
        h_pass(g).wait_send()

    def drain(s, carry):
        for way in range(2):

            @pl.when(jnp.logical_and(has[way], s <= col if way == 0 else s >= col))
            def _(way=way):
                v_line(s, way).wait_send()
                z_line(s, way).wait_send()
                for k in range(slots):
                    x_line(s, k, way).wait_send()

        for f in range(planes - 1):
            z_far(s, f).wait_send()

            @pl.when(jnp.logical_not(jnp.logical_and(middle, jnp.logical_or(s == col - 1, s == col + 1))))
            def _(f=f):
                for k in range(slots):
                    x_far(s, k, f).wait_send()

        for p in range(planes):
            z_twin(s, p).wait_send()
            for k in range(slots):
                x_twin(s, k, p).wait_send()
        for e in range(n_in - 1):
            for j in range(own_j):
                s_peer(s, j, e).wait_send()

        @pl.when(s != col)
        def _():
            for h in range(2):
                m_home(s, h, col).wait_send()

            @pl.when(home == inner)
            def _():
                h_home(s, 0).wait_send()

            @pl.when(helper == inner)
            def _():
                h_relay(s, 0).wait_send()

        return carry

    lax.fori_loop(0, n_col, drain, 0)


def product(flags, u, v, d, x, y, omega, sizes):
    n_row, n_col, n_in = sizes
    slots, js, width = x.shape
    own_j, rank, total = omega.shape
    cols = u.shape[-1]
    planes = n_row // 2
    kr = slots * rank
    group = n_col // n_in
    share = total // n_in
    half = js // 2
    packed = half + rank * (own_j // 2) * rank // (kr + rank)
    vmem = pl.BlockSpec(memory_space=pltpu.VMEM)
    dma = pltpu.SemaphoreType.DMA
    dims = (n_row, n_col, n_in, slots, own_j, rank, width, cols)
    out = jax.ShapeDtypeStruct((own_j, rank, share), WIDE)
    buffers = [
        (u.shape, NARROW),
        ((own_j, rank, width), NARROW),
        ((slots, n_col * js, total), NARROW),
        ((slots, rank, total), NARROW),
        ((slots, js, total), NARROW),
        ((n_in - 1, slots, js, share), NARROW),
        ((slots, total, cols), NARROW),
        ((n_col, own_j, kr, cols), NARROW),
        ((n_col, js, lanes(kr)), NARROW),
        ((js, lanes(kr)), WIDE),
        ((n_row - 1, js // n_row, lanes(kr)), WIDE),
        ((js // n_row, lanes(kr)), NARROW),
        ((n_col, js, cols), WIDE),
        ((n_col, js, cols), NARROW),
        ((n_in - 1, n_col, js, cols), NARROW),
        ((n_col, 2, packed, kr + rank), NARROW),
        ((n_col, 2, packed, kr + rank), NARROW),
        ((n_col, js, cols), NARROW),
        ((group, half, cols), NARROW),
        ((js, share), NARROW),
        ((js, lanes(kr)), WIDE),
        ((js, lanes(kr)), NARROW),
        ((n_in - 1, js, lanes(kr)), NARROW),
        ((own_j, rank, rank), WIDE),
    ]
    held = sum(math.prod(shape) * jnp.dtype(kind).itemsize for shape, kind in buffers)
    return pl.pallas_call(
        functools.partial(product_kernel, dims),
        out_shape=(out, out),
        in_specs=[pl.BlockSpec(memory_space=pltpu.SMEM)] + [pl.BlockSpec(memory_space=pltpu.HBM)] * 6,
        out_specs=[vmem] * 2,
        scratch_shapes=[pltpu.VMEM(*buffer) for buffer in buffers] + [
            dma((2, n_col, slots)), dma((n_col, slots)),
            dma((planes - 1, n_col, slots)), dma((planes - 1, n_col, slots)),
            dma((planes, n_col, slots)), dma((planes, n_col, slots)),
            dma((planes - 1, 2, slots)), dma((planes - 1, 2, slots)),
            dma((2, n_col)), dma((n_col,)),
            dma((2, n_col)), dma((n_col,)),
            dma((planes - 1, n_col)), dma((planes - 1, n_col)),
            dma((planes, n_col)), dma((planes, n_col)),
            dma((n_row - 1,)), dma((n_row - 1,)),
            dma((n_in - 1, n_col, own_j)), dma((n_in - 1, n_col, own_j)),
            dma((n_col, 2)), dma((n_col, 2)),
            dma((n_col,)), dma((group,)),
            dma((n_col,)), dma((group,)),
            dma((group,)), dma((group,)),
            dma((planes - 1, slots)), dma((planes - 1, slots)),
            dma((planes, slots)), dma((planes, slots)),
            dma((n_in - 1, slots)), dma((n_in - 1, slots)),
            dma((n_in - 1, slots)), dma((n_in - 1, slots)),
            dma((n_in - 1,)), dma((n_in - 1,)),
            dma((planes - 1, n_in - 1)), dma((planes - 1, n_in - 1)),
            dma((slots,)), dma((slots,)), dma((slots,)), dma((3,)),
        ],
        compiler_params=pltpu.CompilerParams(
            collective_id=0, has_side_effects=True, vmem_limit_bytes=held + 6 * 1024 * 1024
        ),
    )(flags, *[pltpu.with_memory_space_constraint(part, pltpu.HBM) for part in (u, v, d, x, y, omega)])


def inverse_factor(gram, out_ref):
    count, size = len(gram), gram[0].shape[0]
    tall = lax.broadcasted_iota(jnp.int32, (size, size), 0)
    wide = lax.broadcasted_iota(jnp.int32, (size, size), 1)
    eye = (tall == wide).astype(WIDE)
    lines = lax.broadcasted_iota(jnp.int32, (8, 1), 0)
    works = []
    for j in range(count):
        full = jnp.concatenate([gram[j], eye], axis=1)
        works.append([full[8 * b : 8 * b + 8] for b in range(size // 8)])
    scales = [[] for _ in range(count)]
    for k in range(size):
        b0, in_b = k // 8, k % 8
        for j in range(count):
            work = works[j]
            line = work[b0][in_b : in_b + 1]
            pivot = line[:, k : k + 1]
            scales[j].append(lax.rsqrt(pivot))
            line = line * (1.0 / pivot)
            for b in range(b0, size // 8):
                column = work[b][:, k : k + 1]
                if b == b0:
                    if in_b == 7:
                        continue
                    column = jnp.where(lines > in_b, column, 0.0)
                work[b] = work[b] - column * line
    for j in range(count):
        scale = jnp.concatenate(scales[j], axis=0)
        out_ref[j] = jnp.concatenate(works[j], axis=0)[:, size:] * scale


def local(sizes, near_flags, row_factor, col_factor, near_block, inner_left, inner_right, sketch_matrix):
    slots, own_j, rank, width = inner_left.shape
    js = own_j * rank
    basis, coupling = product(
        near_flags, row_factor[0], col_factor[0], near_block[0],
        inner_left.reshape(slots, js, width), inner_right.reshape(slots, js, width), sketch_matrix, sizes,
    )
    return (basis[None] * math.sqrt(width * sizes[0]), coupling[None])


def solution(mesh):
    sizes = (mesh.shape["row"], mesh.shape["col"], mesh.shape["inner"])
    in_specs = (
        P("row", "inner"),
        P("row", "inner", None, "col"),
        P("row", "inner", None, "col"),
        P("row", "inner", None, "col"),
        P("inner", "col", None, "row"),
        P("inner", "col", None, "row"),
        P("col", None, None),
    )
    out_specs = (P("row", "col", None, "inner"), P("row", "col", None, "inner"))
    return jax.shard_map(
        functools.partial(local, sizes), mesh=mesh, in_specs=in_specs, out_specs=out_specs, check_vma=False
    )
```
